64 devices in a mesh: replica: 4 (over x, y), dp: 16 (over z, core).
Axes of the slice: x: 2, y: 2, z: 8, core: 2. Of those that a mesh axis runs over, the one named last changes fastest.
The devices are a block of a 4x4x8 slice.
Arguments:
- x: bfloat16 [1024, 448], P(('replica', 'dp')), parts along dimension 0
- lengths: int32 [1024], P(('replica', 'dp')), parts along dimension 0
- cache: bfloat16 [2, 1024, 512, 576], P(None, ('replica', 'dp')), parts along dimension 1
- w_q: bfloat16 [2, 448, 2304], replicated
- w_o: bfloat16 [2, 2048, 448], replicated
- expert_ids: int32 [2, 1024, 8], P(None, ('replica', 'dp')), parts along dimension 1
- slots: int32 [2, 1024, 8], P(None, ('replica', 'dp')), parts along dimension 1
- route_w: float32 [2, 1024, 8], P(None, ('replica', 'dp')), parts along dimension 1
- w1_exp: bfloat16 [2, 384, 448, 128], P(None, 'dp')
- w3_exp: bfloat16 [2, 384, 448, 128], P(None, 'dp')
- w2_exp: bfloat16 [2, 384, 128, 448], P(None, 'dp')
- w1_sh: bfloat16 [2, 448, 128], P(None, None, 'dp')
- w3_sh: bfloat16 [2, 448, 128], P(None, None, 'dp')
- w2_sh: bfloat16 [2, 128, 448], P(None, 'dp')
Outputs:
- output: bfloat16 [1024, 448], P(('replica', 'dp')), parts along dimension 0
There are 4 independent parts. The reference program is written for one: setup_inputs(seed, part) draws one part's arguments, and reference() takes and returns one part's arrays. A program takes and returns all parts, laid end to end along the dimension named above; an argument that names none is the same for every part.
All inputs are finite; a program needn't handle non-finite values.
Results may differ from the reference program's by a relative error of at most 0.02.
Values are sent between devices in bfloat16 or wider.
A program may use at most 768 MiB of HBM per device.

```python
import jax
import jax.numpy as jnp
from jax import lax

GROUP_SIZE = 16
BATCH_DEV = 16
SEQ_LEN = 512
D_MODEL = 448
NUM_HEADS = 4
EXPERTS = 384
TOP_K = 8
FF_EXPERT = 128
FF_SHARED = 128
CAPACITY = 1
LAYERS = 2
LATENT = 512
ROPE_DIM = 64

KV_DIM = LATENT + ROPE_DIM
TOKENS = GROUP_SIZE * BATCH_DEV
BUFFER_ROWS = EXPERTS * GROUP_SIZE * CAPACITY
ATT_SCALE = 1.0 / (192.0 ** 0.5)
NORM_EPS = 1e-6


def scaled_normal(key, shape, scale):
    return (jax.random.normal(key, shape, jnp.float32) * scale).astype(jnp.bfloat16)


def draw_routing(key):
    key_bias, key_score, key_hot = jax.random.split(key, 3)
    expert_bias = jax.random.randint(key_bias, (LAYERS, 1, EXPERTS), 0, 512)
    raw_score = jax.random.randint(key_score, (LAYERS, TOKENS, EXPERTS), 0, 1024) + expert_bias
    hot_expert = jax.random.randint(key_hot, (LAYERS, GROUP_SIZE, 1, 1), 0, EXPERTS)
    first_rows = jnp.arange(BATCH_DEV)[None, None, :, None] < CAPACITY
    forced = jnp.logical_and(first_rows, jnp.arange(EXPERTS)[None, None, None, :] == hot_expert)
    raw_score = raw_score + 4096 * forced.astype(jnp.int32).reshape(LAYERS, TOKENS, EXPERTS)
    ranked = raw_score * EXPERTS + jnp.arange(EXPERTS)
    expert_ids = lax.top_k(ranked, TOP_K)[1].astype(jnp.int32)
    member = (expert_ids[:, :, :, None] == jnp.arange(EXPERTS)).astype(jnp.int32)
    member = member.reshape(LAYERS, GROUP_SIZE, BATCH_DEV * TOP_K, EXPERTS)
    slot_rank = jnp.sum(jnp.cumsum(member, axis=2) * member, axis=-1) - 1
    slot_rank = slot_rank.reshape(LAYERS, TOKENS, TOP_K)
    slots = jnp.where(slot_rank < CAPACITY, slot_rank, -1).astype(jnp.int32)
    return expert_ids, slots


def setup_inputs(seed: int = 0, part: int = 0) -> dict:
    part_keys = jax.random.split(jax.random.fold_in(jax.random.key(seed), part), 5)
    weight_keys = jax.random.split(jax.random.key(seed + 1), 8)
    x = scaled_normal(part_keys[0], (TOKENS, D_MODEL), 1.0)
    lengths = jax.random.randint(part_keys[1], (TOKENS,), 1, SEQ_LEN + 1).at[0].set(SEQ_LEN).astype(jnp.int32)
    cache = scaled_normal(part_keys[2], (LAYERS, TOKENS, SEQ_LEN, KV_DIM), 1.0)
    expert_ids, slots = draw_routing(part_keys[3])
    route_w = jax.random.uniform(part_keys[4], (LAYERS, TOKENS, TOP_K), jnp.float32, 0.5, 1.5) * (3.0 / TOP_K)
    return dict(
        x=x,
        lengths=lengths,
        cache=cache,
        w_q=scaled_normal(weight_keys[0], (LAYERS, D_MODEL, NUM_HEADS * KV_DIM), 1.5 * D_MODEL ** -0.5),
        w_o=scaled_normal(weight_keys[1], (LAYERS, NUM_HEADS * LATENT, D_MODEL), (NUM_HEADS * LATENT) ** -0.5),
        expert_ids=expert_ids,
        slots=slots,
        route_w=route_w,
        w1_exp=scaled_normal(weight_keys[2], (LAYERS, EXPERTS, D_MODEL, FF_EXPERT), D_MODEL ** -0.5),
        w3_exp=scaled_normal(weight_keys[3], (LAYERS, EXPERTS, D_MODEL, FF_EXPERT), D_MODEL ** -0.5),
        w2_exp=scaled_normal(weight_keys[4], (LAYERS, EXPERTS, FF_EXPERT, D_MODEL), 1.5 * FF_EXPERT ** -0.5),
        w1_sh=scaled_normal(weight_keys[5], (LAYERS, D_MODEL, FF_SHARED), D_MODEL ** -0.5),
        w3_sh=scaled_normal(weight_keys[6], (LAYERS, D_MODEL, FF_SHARED), D_MODEL ** -0.5),
        w2_sh=scaled_normal(weight_keys[7], (LAYERS, FF_SHARED, D_MODEL), 2.0 * FF_SHARED ** -0.5),
    )


def rms_norm(values):
    vals32 = values.astype(jnp.float32)
    return vals32 * lax.rsqrt(jnp.mean(vals32 * vals32, axis=-1, keepdims=True) + NORM_EPS)


def attend_block(block_args):
    q_block, cache_block, len_block = block_args
    scores = jnp.einsum('bhc,btc->bht', q_block.astype(jnp.float32), cache_block.astype(jnp.float32)) * ATT_SCALE
    valid = jnp.arange(SEQ_LEN)[None, None, :] < len_block[:, None, None]
    probs = jax.nn.softmax(jnp.where(valid, scores, -jnp.inf), axis=-1)
    probs = probs.astype(jnp.bfloat16).astype(jnp.float32)
    return jnp.einsum('bht,btc->bhc', probs, cache_block[:, :, :LATENT].astype(jnp.float32))


def reference(x, lengths, cache, w_q, w_o, expert_ids, slots, route_w, w1_exp, w3_exp, w2_exp, w1_sh, w3_sh, w2_sh):
    owner_dev = jnp.arange(TOKENS) // BATCH_DEV
    len_blocks = lengths.reshape(GROUP_SIZE, BATCH_DEV)

    def layer_step(resid, layer_args):
        cache_l, w_q_l, w_o_l, ids_l, slot_l, gate_w, w1_e, w3_e, w2_e, w1_s, w3_s, w2_s = layer_args
        normed = rms_norm(resid).astype(jnp.bfloat16)
        queries = jnp.dot(normed, w_q_l, preferred_element_type=jnp.float32).astype(jnp.bfloat16)
        queries = queries.reshape(GROUP_SIZE, BATCH_DEV, NUM_HEADS, KV_DIM)
        attn = lax.map(attend_block, (queries, cache_l.reshape(GROUP_SIZE, BATCH_DEV, SEQ_LEN, KV_DIM), len_blocks))
        attn = attn.astype(jnp.bfloat16).reshape(TOKENS, NUM_HEADS * LATENT)
        resid = (resid.astype(jnp.float32) + jnp.dot(attn, w_o_l, preferred_element_type=jnp.float32)).astype(jnp.bfloat16)
        ffn_in = rms_norm(resid).astype(jnp.bfloat16)
        shared_gate = jnp.dot(ffn_in, w3_s, preferred_element_type=jnp.float32)
        shared_up = jnp.dot(ffn_in, w1_s, preferred_element_type=jnp.float32)
        shared_h = (jax.nn.silu(shared_gate) * shared_up).astype(jnp.bfloat16)
        shared_out = jnp.dot(shared_h, w2_s, preferred_element_type=jnp.float32)
        buf_rows = jnp.where(slot_l >= 0, ids_l * (GROUP_SIZE * CAPACITY) + owner_dev[:, None] * CAPACITY + slot_l, BUFFER_ROWS)
        copies = jnp.broadcast_to(ffn_in[:, None, :], (TOKENS, TOP_K, D_MODEL)).reshape(TOKENS * TOP_K, D_MODEL)
        buffer = jnp.zeros((BUFFER_ROWS, D_MODEL), jnp.bfloat16).at[buf_rows.reshape(-1)].set(copies, mode='drop')
        buffer = buffer.reshape(EXPERTS, GROUP_SIZE * CAPACITY, D_MODEL).astype(jnp.float32)
        gate_in = jnp.einsum('ecd,edf->ecf', buffer, w3_e.astype(jnp.float32))
        up_in = jnp.einsum('ecd,edf->ecf', buffer, w1_e.astype(jnp.float32))
        hidden = (jax.nn.silu(gate_in) * up_in).astype(jnp.bfloat16).astype(jnp.float32)
        expert_out = jnp.einsum('ecf,efd->ecd', hidden, w2_e.astype(jnp.float32)).astype(jnp.bfloat16)
        picked = jnp.take(expert_out.reshape(BUFFER_ROWS, D_MODEL), buf_rows, axis=0, mode='fill', fill_value=0)
        routed = jnp.sum(gate_w[:, :, None] * picked.astype(jnp.float32), axis=1)
        resid = (resid.astype(jnp.float32) + routed + shared_out).astype(jnp.bfloat16)
        return resid, None

    final_x = lax.scan(layer_step, x, (cache, w_q, w_o, expert_ids, slots, route_w, w1_exp, w3_exp, w2_exp, w1_sh, w3_sh, w2_sh))[0]
    return final_x
```

```python
import functools

import jax
import jax.numpy as jnp
from jax import lax
from jax.experimental import pallas as pl
from jax.experimental.pallas import tpu as pltpu
from jax.sharding import PartitionSpec as P

NORM_EPS = 1e-6
ATT_SCALE = 1.0 / (192.0 ** 0.5)
LATENT = 512
MESH = pl.DeviceIdType.MESH
F32 = jnp.float32
BF16 = jnp.bfloat16


def rms_norm(vals32):
    return vals32 * lax.rsqrt(jnp.mean(vals32 * vals32, axis=-1, keepdims=True) + NORM_EPS)


def dot(lhs, rhs):
    return jnp.dot(lhs, rhs, preferred_element_type=F32)


def dot_t(lhs, rhs):
    return lax.dot_general(lhs, rhs, (((1,), (1,)), ((), ())), preferred_element_type=F32)


def step_kernel(chips, len_ref, x_hbm, cache_hbm, wq_hbm, wo_hbm, ids_hbm, slots_hbm, rw_hbm, w1_hbm, w3_hbm, w2_hbm,
                w1s_hbm, w3s_hbm, w2s_hbm, out_ref,
                x_v, cache_v, wq_v, wo_v, ids_v, slots_v, rw_v, w1_v, w3_v, w2_v, w1s_v, w3s_v, w2s_v,
                rp_all, oh_v, owt_v, g_all, p_buf, r1_buf, s_buf, r2_buf,
                q_v, sc_v, pr_v, o_v, xg_v, u_v,
                loc_sem, cache_sem, ag_send, ag_recv, fwd_send, rs1_send, rs1_recv, rs2_send, rs2_recv):
    layers, bat, kv_dim, seq_len = cache_v.shape
    d_model = x_v.shape[1]
    heads = wq_v.shape[2] // kv_dim
    rows = heads * bat
    n_exp = w1_v.shape[1]
    ff = w1_v.shape[3]
    top_k = ids_v.shape[1]
    group = 2 * chips
    toks = group * bat
    half = chips * bat

    me = lax.axis_index('dp')
    chip = me // 2
    core = me % 2
    other = 1 - core
    q_me = core * chips + chip
    partner = me + 1 - 2 * core

    far_first = (4, 3, 5, 2, 6, 1, 7)
    near_first = (1, 7, 2, 6, 3, 5, 4)

    def chip_at(delta):
        return lax.rem(chip + delta, chips)

    barrier = pltpu.get_barrier_semaphore()
    for delta in far_first:
        pl.semaphore_signal(barrier, inc=1, device_id={'dp': 2 * chip_at(delta) + core}, device_id_type=MESH)
    pl.semaphore_signal(barrier, inc=1, device_id={'dp': partner}, device_id_type=MESH)

    def load(src, dst, idx):
        return pltpu.make_async_copy(src, dst, loc_sem.at[idx])

    small = [load(x_hbm, x_v, 0), load(ids_hbm, ids_v, 1), load(slots_hbm, slots_v, 2), load(rw_hbm, rw_v, 3),
             load(w1s_hbm, w1s_v, 4), load(w3s_hbm, w3s_v, 5), load(w2s_hbm, w2s_v, 6)]
    wq_cp = [load(wq_hbm.at[l], wq_v.at[l], 7 + l) for l in range(layers)]
    wo_cp = [load(wo_hbm.at[l], wo_v.at[l], 9 + l) for l in range(layers)]
    w3_cp = [load(w3_hbm.at[l], w3_v.at[l], 11 + l) for l in range(layers)]
    w1_cp = [load(w1_hbm.at[l], w1_v.at[l], 13 + l) for l in range(layers)]
    w2_cp = [load(w2_hbm.at[l], w2_v.at[l], 15 + l) for l in range(layers)]

    def cache_cp(l, b):
        return pltpu.make_async_copy(cache_hbm.at[l, b], cache_v.at[l, b], cache_sem.at[l, b])

    small[0].start()
    wq_cp[0].start()
    for cp in small[1:4]:
        cp.start()
    for b in range(bat):
        cache_cp(0, b).start()
    for cp in small[4:]:
        cp.start()
    wo_cp[0].start()

    def remote(src, dst, send, recv, dev):
        return pltpu.make_async_remote_copy(src_ref=src, dst_ref=dst, send_sem=send, recv_sem=recv,
                                            device_id={'dp': dev}, device_id_type=MESH)

    def ag_copies(buf, ph):
        mine = buf.at[q_me]
        cps = [remote(mine, mine, ag_send.at[ph, i], ag_recv.at[ph, q_me], 2 * chip_at(delta) + core)
               for i, delta in enumerate(far_first)]
        cps.append(remote(mine, mine, ag_send.at[ph, chips - 1], ag_recv.at[ph, q_me], partner))
        return cps

    def ag_start(buf, ph):
        cps = ag_copies(buf, ph)
        for cp in cps:
            cp.start()
        return cps

    def ag_finish(buf, ph, cps):
        fwd = []
        for i, delta in enumerate(near_first):
            q = core * chips + chip_at(chips - delta)
            cp = remote(buf.at[q], buf.at[q], fwd_send.at[ph, i], ag_recv.at[ph, q], partner)
            cp.wait_recv()
            cp.start()
            fwd.append(cp)
        for delta in (0,) + near_first:
            q = other * chips + chip_at(chips - delta)
            remote(buf.at[q], buf.at[q], fwd_send.at[ph, 0], ag_recv.at[ph, q], partner).wait_recv()
        for cp in cps + fwd:
            cp.wait_send()

    row_tok = lax.rem(lax.broadcasted_iota(jnp.int32, (rows, 1), 0), bat)

    for cp in small[1:4]:
        cp.wait()
    pieces = []
    for l in range(layers):
        pieces.append(jnp.where(slots_v[l] >= 0, ids_v[l] + 1, 0).astype(F32))
    for l in range(layers):
        pieces.append(rw_v[l])
    packed = jnp.concatenate(pieces, axis=0)
    packed = jnp.concatenate([packed, jnp.zeros((2 * layers * top_k, half - bat), F32)], axis=1)
    rp_all[q_me] = pltpu.roll(packed, chip * bat, 1)

    pl.semaphore_wait(barrier, chips)
    rp_cps = ag_start(rp_all, layers)

    small[0].wait()

    def attention(l):
        hidden = rms_norm(x_v[...].astype(F32)).astype(BF16)
        wq_cp[l].wait()
        q = dot(hidden, wq_v[l])
        for hd in range(heads):
            part = q if hd == 0 else pltpu.roll(q, heads * kv_dim - hd * kv_dim, 1)
            q_v[hd * bat:(hd + 1) * bat, :] = part[:, :kv_dim].astype(BF16)
        q_all = q_v[...]
        sc_v[...] = jnp.zeros(sc_v.shape, F32)

        def score_step(g, carry):
            acc = None
            for i in range(4):
                b = 4 * g + i
                cache_cp(l, b).wait()
                qm = q_all * (row_tok == b).astype(F32).astype(BF16)
                term = dot(qm, cache_v[l, b])
                acc = term if acc is None else acc + term
            sc_v[...] += acc
            return carry

        lax.fori_loop(0, bat // 4, score_step, 0)
        if l == 0:
            for cps in (w3_cp, w1_cp, w2_cp):
                cps[0].start()
        lens = jnp.zeros((rows, 1), jnp.int32)
        for b in range(bat):
            lens = jnp.where(row_tok == b, len_ref[b], lens)
        valid = lax.broadcasted_iota(jnp.int32, (rows, seq_len), 1) < lens
        scores = jnp.where(valid, sc_v[...] * ATT_SCALE, -jnp.inf)
        top = jnp.max(scores, axis=1, keepdims=True)
        ex = jnp.exp(scores - top)
        probs = (ex / jnp.sum(ex, axis=1, keepdims=True)).astype(BF16)
        o_v[...] = jnp.zeros(o_v.shape, F32)

        def out_step(g, carry):
            acc = None
            for i in range(4):
                b = 4 * g + i
                pm = probs * (row_tok == b).astype(F32).astype(BF16)
                term = dot_t(pm, cache_v[l, b, 0:LATENT, :])
                acc = term if acc is None else acc + term
            o_v[...] += acc
            return carry

        lax.fori_loop(0, bat // 4, out_step, 0)
        attn = jnp.concatenate([o_v[hd * bat:(hd + 1) * bat, :].astype(BF16) for hd in range(heads)], axis=1)
        wo_cp[l].wait()
        return (x_v[...].astype(F32) + dot_t(attn, wo_v[l])).astype(BF16)

    def build_masks():
        code_w = []
        for k in range(2):
            tot = rp_all[k * chips]
            for j in range(1, chips):
                tot = tot + rp_all[k * chips + j]
            code_w.append(tot)
        code_w = jnp.concatenate(code_w, axis=1)
        base = me * n_exp + 1
        exp_iota = lax.broadcasted_iota(jnp.int32, (n_exp, toks), 0)
        want = (exp_iota + base).astype(F32)
        lane_src = lax.broadcasted_iota(jnp.int32, (group, toks), 1) // bat
        own_src = lane_src == lax.broadcasted_iota(jnp.int32, (group, toks), 0)
        for l in range(layers):
            member = jnp.zeros((n_exp, toks), F32)
            weight = jnp.zeros((n_exp, toks), F32)
            for j in range(top_k):
                hit = code_w[l * top_k + j:l * top_k + j + 1, :] == want
                member = jnp.where(hit, 1.0, member)
                wrow = code_w[(layers + l) * top_k + j:(layers + l) * top_k + j + 1, :]
                weight = jnp.where(hit, wrow, weight)
            onehot = [jnp.where(own_src, member[n:n + 1, :], 0.0) for n in range(n_exp)]
            oh_v[l] = jnp.concatenate(onehot, axis=0).astype(BF16)
            ow = jnp.concatenate([jnp.where(own_src, weight[n:n + 1, :], 0.0) for n in range(n_exp)], axis=0)
            owt = ow.T
            hi = owt.astype(BF16)
            rest = owt - hi.astype(F32)
            mid = rest.astype(BF16)
            low = (rest - mid.astype(F32)).astype(BF16)
            owt_v[l, 0] = hi
            owt_v[l, 1] = mid
            owt_v[l, 2] = low

    def experts(l):
        g_in = g_all[l].reshape(toks, d_model)
        xg_v[...] = dot(oh_v[l], g_in).astype(BF16)
        gate = dot_t(g_in, w3s_v[l])
        up = dot_t(g_in, w1s_v[l])
        shared_h = (jax.nn.silu(gate) * up).astype(BF16)
        shared = dot(shared_h, w2s_v[l])

        for cps in (w3_cp, w1_cp, w2_cp):
            cps[l].wait()

        def pair_step(i, carry):
            for jj in range(2):
                pair = 2 * i + jj
                hid = []
                for e in range(2):
                    n = 2 * pair + e
                    start = pl.multiple_of(n * group, group)
                    xin = xg_v[pl.ds(start, group), :]
                    w31 = jnp.concatenate([w3_v[l, n], w1_v[l, n]], axis=1)
                    both = dot(xin, w31)
                    hid.append((jax.nn.silu(both[:, :ff]) * both[:, ff:]).astype(BF16))
                zero = jnp.zeros((group, ff), BF16)
                lhs = jnp.concatenate([jnp.concatenate([hid[0], zero], axis=1),
                                       jnp.concatenate([zero, hid[1]], axis=1)], axis=0)
                w2p = jnp.concatenate([w2_v[l, 2 * pair], w2_v[l, 2 * pair + 1]], axis=1)
                start = pl.multiple_of(pair * 2 * group, 2 * group)
                u_v[pl.ds(start, 2 * group), :] = dot_t(lhs, w2p).astype(BF16)
            return carry

        lax.fori_loop(0, n_exp // 4, pair_step, 0)
        u_in = u_v[...]
        total = shared + (dot(owt_v[l, 0], u_in) + dot(owt_v[l, 1], u_in) + dot(owt_v[l, 2], u_in))
        p_buf[l] = total.reshape(group, bat, d_model)

    def combine(l):
        first = remote(p_buf.at[l, pl.ds(other * chips, chips)], r1_buf.at[l], rs1_send.at[l], rs1_recv.at[l], partner)
        first.start()
        first.wait_recv()
        s_buf[l] = p_buf[l, pl.ds(core * chips, chips)] + r1_buf[l]
        cps = []
        for i, delta in enumerate(far_first):
            dst = chip_at(delta)
            cps.append(remote(s_buf.at[l, dst], r2_buf.at[l, chip], rs2_send.at[l, i], rs2_recv.at[l, chip], 2 * dst + core))
        for cp in cps:
            cp.start()
        r2_buf[l, chip] = s_buf[l, chip]
        for i, delta in enumerate(near_first):
            src = chip_at(chips - delta)
            remote(s_buf.at[l, src], r2_buf.at[l, src], rs2_send.at[l, 0], rs2_recv.at[l, src], partner).wait_recv()
        tot = r2_buf[l, 0]
        for j in range(1, chips):
            tot = tot + r2_buf[l, j]
        first.wait_send()
        for cp in cps:
            cp.wait_send()
        return tot

    for l in range(layers):
        resid = attention(l)
        g_all[l, q_me] = rms_norm(resid.astype(F32)).astype(BF16)
        cps = ag_start(g_all.at[l], l)
        if l == 0:
            for cp in small[4:]:
                cp.wait()
            wq_cp[1].start()
            for b in range(bat):
                cache_cp(1, b).start()
            for cp_list in (wo_cp, w3_cp, w1_cp, w2_cp):
                cp_list[1].start()
            ag_finish(rp_all, layers, rp_cps)
            build_masks()
        ag_finish(g_all.at[l], l, cps)
        experts(l)
        x_v[...] = (resid.astype(F32) + combine(l)).astype(BF16)
    out_ref[...] = x_v[...]


def solution(mesh):
    group = mesh.shape['dp']
    chips = group // 2
    tok_axes = ('replica', 'dp')
    in_specs = (
        P(tok_axes, None), P(tok_axes), P(None, tok_axes, None, None),
        P(None, None, None), P(None, None, None),
        P(None, tok_axes, None), P(None, tok_axes, None), P(None, tok_axes, None),
        P(None, 'dp', None, None), P(None, 'dp', None, None), P(None, 'dp', None, None),
        P(None, None, 'dp'), P(None, None, 'dp'), P(None, 'dp', None),
    )

    def device_step(x, lengths, cache, w_q, w_o, expert_ids, slots, route_w, w1_exp, w3_exp, w2_exp, w1_sh, w3_sh, w2_sh):
        bat, d_model = x.shape
        layers, _, seq_len, kv_dim = cache.shape
        n_exp, ff = w1_exp.shape[1], w1_exp.shape[3]
        top_k = expert_ids.shape[2]
        heads = w_q.shape[2] // kv_dim
        assert max(1, (2 * bat * top_k) // (n_exp * group)) == 1 and layers == 2 and chips == 8
        swap = lambda a: jnp.swapaxes(a, -1, -2)
        args = (lengths, x, swap(cache), w_q, swap(w_o), swap(expert_ids), swap(slots), swap(route_w),
                w1_exp, w3_exp, swap(w2_exp), swap(w1_sh), swap(w3_sh), w2_sh)
        vm = lambda a: pltpu.VMEM(a.shape, a.dtype)
        toks = group * bat
        dma = pltpu.SemaphoreType.DMA
        scratch = [vm(a) for a in args[1:]] + [
            pltpu.VMEM((group, 2 * layers * top_k, chips * bat), F32),
            pltpu.VMEM((layers, n_exp * group, toks), BF16),
            pltpu.VMEM((layers, 3, toks, n_exp * group), BF16),
            pltpu.VMEM((layers, group, bat, d_model), BF16),
            pltpu.VMEM((layers, group, bat, d_model), F32),
            pltpu.VMEM((layers, chips, bat, d_model), F32),
            pltpu.VMEM((layers, chips, bat, d_model), F32),
            pltpu.VMEM((layers, chips, bat, d_model), F32),
            pltpu.VMEM((heads * bat, kv_dim), BF16),
            pltpu.VMEM((heads * bat, seq_len), F32),
            pltpu.VMEM((heads * bat, seq_len), BF16),
            pltpu.VMEM((heads * bat, LATENT), F32),
            pltpu.VMEM((n_exp * group, d_model), BF16),
            pltpu.VMEM((n_exp * group, d_model), BF16),
            dma((17,)), dma((layers, bat)),
            dma((layers + 1, chips)), dma((layers + 1, group)), dma((layers + 1, chips)),
            dma((layers,)), dma((layers,)), dma((layers, chips)), dma((layers, chips)),
        ]
        return pl.pallas_call(
            functools.partial(step_kernel, chips),
            out_shape=jax.ShapeDtypeStruct(x.shape, x.dtype),
            in_specs=[pl.BlockSpec(memory_space=pltpu.SMEM)] + [pl.BlockSpec(memory_space=pl.ANY)] * (len(args) - 1),
            out_specs=pl.BlockSpec(memory_space=pltpu.VMEM),
            scratch_shapes=scratch,
            compiler_params=pltpu.CompilerParams(collective_id=0, has_side_effects=True, vmem_limit_bytes=67043328),
        )(*args)

    return jax.shard_map(device_step, mesh=mesh, in_specs=in_specs, out_specs=P(tok_axes, None), check_vma=False)
```

```python
import functools

import jax
import jax.numpy as jnp
from jax import lax
from jax.experimental import pallas as pl
from jax.experimental.pallas import tpu as pltpu
from jax.sharding import PartitionSpec as P

NORM_EPS = 1e-6
ATT_SCALE = 1.0 / (192.0 ** 0.5)
LATENT = 512
MESH = pl.DeviceIdType.MESH
F32 = jnp.float32
BF16 = jnp.bfloat16


def rms_norm(vals32):
    return vals32 * lax.rsqrt(jnp.mean(vals32 * vals32, axis=-1, keepdims=True) + NORM_EPS)


def dot(lhs, rhs):
    return jnp.dot(lhs, rhs, preferred_element_type=F32)


def dot_t(lhs, rhs):
    return lax.dot_general(lhs, rhs, (((1,), (1,)), ((), ())), preferred_element_type=F32)


def step_kernel(chips, len_ref, x_hbm, cache_hbm, wq_hbm, wo_hbm, ids_hbm, slots_hbm, rw_hbm, w1_hbm, w3_hbm, w2_hbm,
                w1s_hbm, w3s_hbm, w2s_hbm, out_ref,
                x_v, cache_v, wq_v, wo_v, ids_v, slots_v, rw_v, w1_v, w3_v, w2_v, w1s_v, w3s_v, w2s_v,
                rp_all, oh_v, owt_v, g_all, p_buf, own_buf, r1_buf, s_buf, r2_buf,
                xr_v, wot_v, q_v, sc_v, o_v, xg_v, u_v, sh_v,
                loc_sem, cache_sem, ag_send, ag_recv, fwd_send, rs1_send, rs1_recv, rs2_send, rs2_recv):
    layers, bat, kv_dim, seq_len = cache_v.shape
    d_model = x_v.shape[1]
    heads = wq_v.shape[2] // kv_dim
    n_exp = w1_v.shape[1]
    ff = w1_v.shape[3]
    top_k = ids_v.shape[1]
    group = 2 * chips
    hb = bat // 2
    rows = heads * hb
    toks = group * hb
    half = chips * hb
    quad = 4

    me = lax.axis_index('dp')
    chip = me // 2
    core = me % 2
    other = 1 - core
    q_me = core * chips + chip
    partner = me + 1 - 2 * core

    far_first = (4, 3, 5, 2, 6, 1, 7)
    near_first = (1, 7, 2, 6, 3, 5, 4)

    def chip_at(delta):
        return lax.rem(chip + delta, chips)

    barrier = pltpu.get_barrier_semaphore()
    for delta in far_first:
        pl.semaphore_signal(barrier, inc=1, device_id={'dp': 2 * chip_at(delta) + core}, device_id_type=MESH)
    pl.semaphore_signal(barrier, inc=1, device_id={'dp': partner}, device_id_type=MESH)

    def load(src, dst, idx):
        return pltpu.make_async_copy(src, dst, loc_sem.at[idx])

    small = [load(x_hbm, x_v, 0), load(ids_hbm, ids_v, 1), load(slots_hbm, slots_v, 2), load(rw_hbm, rw_v, 3),
             load(w1s_hbm, w1s_v, 4), load(w3s_hbm, w3s_v, 5), load(w2s_hbm, w2s_v, 6)]
    wq_cp = [load(wq_hbm.at[l], wq_v.at[l], 7 + l) for l in range(layers)]
    wo_cp = [load(wo_hbm.at[l], wo_v.at[l], 9 + l) for l in range(layers)]
    w3_cp = [load(w3_hbm.at[l], w3_v.at[l], 11 + l) for l in range(layers)]
    w1_cp = [load(w1_hbm.at[l], w1_v.at[l], 13 + l) for l in range(layers)]
    w2_cp = [load(w2_hbm.at[l], w2_v.at[l], 15 + l) for l in range(layers)]
    cache_cp = [[pltpu.make_async_copy(cache_hbm.at[l, pl.ds(quad * c, quad)], cache_v.at[l, pl.ds(quad * c, quad)],
                                       cache_sem.at[l, c]) for c in range(bat // quad)] for l in range(layers)]

    small[0].start()
    wq_cp[0].start()
    for cp in small[1:4]:
        cp.start()
    cache_cp[0][0].start()
    wo_cp[0].start()
    for cp in cache_cp[0][1:]:
        cp.start()
    for cp in small[4:]:
        cp.start()

    def remote(src, dst, send, recv, dev):
        return pltpu.make_async_remote_copy(src_ref=src, dst_ref=dst, send_sem=send, recv_sem=recv,
                                            device_id={'dp': dev}, device_id_type=MESH)

    def ag_start(buf, ph):
        mine = buf.at[q_me]
        cps = [remote(mine, mine, ag_send.at[ph, i], ag_recv.at[ph, q_me], 2 * chip_at(delta) + core)
               for i, delta in enumerate(far_first)]
        cps.append(remote(mine, mine, ag_send.at[ph, chips - 1], ag_recv.at[ph, q_me], partner))
        for cp in cps:
            cp.start()
        return cps

    def ag_finish(buf, ph):
        fwd = []
        for i, delta in enumerate(near_first):
            q = core * chips + chip_at(chips - delta)
            cp = remote(buf.at[q], buf.at[q], fwd_send.at[ph, i], ag_recv.at[ph, q], partner)
            cp.wait_recv()
            cp.start()
            fwd.append(cp)
        for delta in (0,) + near_first:
            q = other * chips + chip_at(chips - delta)
            remote(buf.at[q], buf.at[q], fwd_send.at[ph, 0], ag_recv.at[ph, q], partner).wait_recv()
        return fwd

    for cp in small[1:4]:
        cp.wait()
    pieces = []
    for l in range(layers):
        pieces.append(jnp.where(slots_v[l] >= 0, ids_v[l] + 1, 0).astype(F32))
    for l in range(layers):
        pieces.append(rw_v[l])
    packed = jnp.concatenate(pieces, axis=0)
    packed = jnp.concatenate([packed, jnp.zeros((2 * layers * top_k, toks - bat), F32)], axis=1)
    lane = lax.broadcasted_iota(jnp.int32, packed.shape, 1)
    rp_all[q_me, 0] = pltpu.roll(jnp.where(lane < hb, packed, 0.0), q_me * hb, 1)
    second = jnp.where(lane < hb, pltpu.roll(packed, toks - hb, 1), 0.0)
    rp_all[q_me, 1] = pltpu.roll(second, q_me * hb, 1)

    pl.semaphore_wait(barrier, chips)
    sends = ag_start(rp_all, 2 * layers)

    small[0].wait()
    xr_v[...] = x_v[...].astype(F32).reshape(2, hb, d_model)

    def transpose_wo(l):
        wo_cp[l].wait()
        for k in range(heads * LATENT // 128):
            wot_v[l, 128 * k:128 * (k + 1), :] = wo_v[l, :, 128 * k:128 * (k + 1)].T

    def attention(l, hf):
        hidden = rms_norm(xr_v[hf]).astype(BF16)
        if hf == 0:
            wq_cp[l].wait()
        q = dot(hidden, wq_v[l])
        for hd in range(heads):
            part = q if hd == 0 else pltpu.roll(q, heads * kv_dim - hd * kv_dim, 1)
            for k in range(q_v.shape[0]):
                q_v[k, pl.ds(hd, hb, stride=heads), :] = part[:, 128 * k:128 * (k + 1)]
        for c in range(2):
            cache_cp[l][2 * hf + c].wait()
            for i in range(quad):
                b = quad * c + i
                qb = jnp.concatenate([q_v[k, heads * b:heads * (b + 1), :] for k in range(q_v.shape[0])], axis=1)
                qb = qb[:, :kv_dim].astype(BF16)
                sc_v[heads * b:heads * (b + 1), :] = dot(qb, cache_v[l, hf * hb + b])
            if l == 0 and hf == 0 and c == 0:
                transpose_wo(0)
        if l == 0 and hf == 0:
            for cps in (w3_cp, w1_cp, w2_cp):
                cps[0].start()
        row_tok = lax.broadcasted_iota(jnp.int32, (rows, 1), 0) // heads
        lens = jnp.zeros((rows, 1), jnp.int32)
        for b in range(hb):
            lens = jnp.where(row_tok == b, len_ref[hf * hb + b], lens)
        valid = lax.broadcasted_iota(jnp.int32, (rows, seq_len), 1) < lens
        scores = jnp.where(valid, sc_v[...] * ATT_SCALE, -jnp.inf)
        top = jnp.max(scores, axis=1, keepdims=True)
        ex = jnp.exp(scores - top)
        probs = ex / jnp.sum(ex, axis=1, keepdims=True)
        sc_v[...] = probs
        for b in range(hb):
            pb = sc_v[heads * b:heads * (b + 1), :].astype(BF16)
            ob = dot_t(pb, cache_v[l, hf * hb + b, 0:LATENT, :])
            for k in range(o_v.shape[0]):
                o_v[k, heads * b:heads * (b + 1), :] = ob[:, 128 * k:128 * (k + 1)]
        attn = jnp.concatenate([o_v[k, pl.ds(hd, hb, stride=heads), :] for hd in range(heads)
                                for k in range(o_v.shape[0])], axis=1).astype(BF16)
        proj = jnp.concatenate([dot(attn, wot_v[l, :, 0:256]), dot(attn, wot_v[l, :, 256:d_model])], axis=1)
        resid = (xr_v[hf] + proj).astype(BF16).astype(F32)
        xr_v[hf] = resid
        g_all[2 * l + hf, q_me] = rms_norm(resid).astype(BF16)

    def build_masks(l):
        base = me * n_exp + 1
        want = (lax.broadcasted_iota(jnp.int32, (n_exp, toks), 0) + base).astype(F32)
        lane_src = lax.broadcasted_iota(jnp.int32, (group, toks), 1) // hb
        own_src = lane_src == lax.broadcasted_iota(jnp.int32, (group, toks), 0)
        for hf in range(2):
            code = rp_all[0, hf, l * top_k:(l + 1) * top_k, :]
            wval = rp_all[0, hf, (layers + l) * top_k:(layers + l + 1) * top_k, :]
            for j in range(1, group):
                code = code + rp_all[j, hf, l * top_k:(l + 1) * top_k, :]
                wval = wval + rp_all[j, hf, (layers + l) * top_k:(layers + l + 1) * top_k, :]
            member = jnp.zeros((n_exp, toks), F32)
            weight = jnp.zeros((n_exp, toks), F32)
            for j in range(top_k):
                hit = code[j:j + 1, :] == want
                member = jnp.where(hit, 1.0, member)
                weight = jnp.where(hit, wval[j:j + 1, :], weight)
            onehot = [jnp.where(own_src, member[n:n + 1, :], 0.0) for n in range(n_exp)]
            oh_v[l, hf] = jnp.concatenate(onehot, axis=0).astype(BF16)
            ow = jnp.concatenate([jnp.where(own_src, weight[n:n + 1, :], 0.0) for n in range(n_exp)], axis=0)
            owt = ow.T
            hi = owt.astype(BF16)
            rest = owt - hi.astype(F32)
            mid = rest.astype(BF16)
            low = (rest - mid.astype(F32)).astype(BF16)
            owt_v[l, hf, 0] = hi
            owt_v[l, hf, 1] = mid
            owt_v[l, hf, 2] = low

    unroll = 4

    def experts(l, hf, between=None):
        ph = 2 * l + hf
        g_in = g_all[ph].reshape(toks, d_model)
        xg_v[...] = dot(oh_v[l, hf], g_in).astype(BF16)
        gate = dot_t(g_in, w3s_v[l])
        up = dot_t(g_in, w1s_v[l])
        shared_h = (jax.nn.silu(gate) * up).astype(BF16)
        sh_v[...] = dot(shared_h, w2s_v[l])
        if hf == 0:
            for cps in (w3_cp, w1_cp, w2_cp):
                cps[l].wait()

        def first_layer(pair):
            hid = []
            for e in range(2):
                n = 2 * pair + e
                start = pl.multiple_of(n * group, group)
                xin = xg_v[pl.ds(start, group), :]
                w31 = jnp.concatenate([w3_v[l, n], w1_v[l, n]], axis=1)
                both = dot(xin, w31)
                hid.append((jax.nn.silu(both[:, :ff]) * both[:, ff:]).astype(BF16))
            zero = jnp.zeros((group, ff), BF16)
            return jnp.concatenate([jnp.concatenate([hid[0], zero], axis=1),
                                    jnp.concatenate([zero, hid[1]], axis=1)], axis=0)

        def second_layer(pair, lhs):
            w2p = jnp.concatenate([w2_v[l, 2 * pair], w2_v[l, 2 * pair + 1]], axis=1)
            start = pl.multiple_of(pair * 2 * group, 2 * group)
            u_v[pl.ds(start, 2 * group), :] = dot_t(lhs, w2p).astype(BF16)

        def pair_step(i, carry):
            ready = first_layer(unroll * i)
            for jj in range(unroll):
                pair = unroll * i + jj
                coming = first_layer(pair + 1) if jj < unroll - 1 else None
                second_layer(pair, ready)
                ready = coming
            return carry

        steps = n_exp // (2 * unroll)
        lax.fori_loop(0, 1, pair_step, 0)
        if between is not None:
            between()
        lax.fori_loop(1, steps, pair_step, 0)

        def part(k):
            sel = pl.ds(pl.multiple_of(k * half, half), half)
            u_in = u_v[...]
            return sh_v[sel, :] + (dot(owt_v[l, hf, 0, sel, :], u_in) + dot(owt_v[l, hf, 1, sel, :], u_in)
                                   + dot(owt_v[l, hf, 2, sel, :], u_in))

        p_buf[ph] = part(other).reshape(chips, hb, d_model)
        first = remote(p_buf.at[ph], r1_buf.at[ph], rs1_send.at[ph], rs1_recv.at[ph], partner)
        first.start()
        own_buf[ph] = part(core).reshape(chips, hb, d_model)
        return first

    def second_stage(l, hf, first):
        ph = 2 * l + hf
        first.wait_recv()
        s_buf[ph] = own_buf[ph] + r1_buf[ph]
        cps = [first]
        for i, delta in enumerate(far_first):
            dst = chip_at(delta)
            cp = remote(s_buf.at[ph, dst], r2_buf.at[ph, chip], rs2_send.at[ph, i], rs2_recv.at[ph, chip], 2 * dst + core)
            cp.start()
            cps.append(cp)
        r2_buf[ph, chip] = s_buf[ph, chip]
        return cps

    def finish(l, hf):
        ph = 2 * l + hf
        for i, delta in enumerate(near_first):
            src = chip_at(chips - delta)
            remote(s_buf.at[ph, src], r2_buf.at[ph, src], rs2_send.at[ph, 0], rs2_recv.at[ph, src], partner).wait_recv()
        tot = r2_buf[ph, 0]
        for j in range(1, chips):
            tot = tot + r2_buf[ph, j]
        xr_v[hf] = (xr_v[hf] + tot).astype(BF16).astype(F32)

    for l in range(layers):
        for hf in range(2):
            if l > 0:
                finish(l - 1, hf)
            attention(l, hf)
            sends += ag_start(g_all.at[2 * l + hf], 2 * l + hf)
            if l == 0 and hf == 0:
                wq_cp[1].start()
                for cp in cache_cp[1]:
                    cp.start()
        if l == 0:
            for cp_list in (wo_cp, w3_cp, w1_cp, w2_cp):
                cp_list[1].start()
            for cp in small[4:]:
                cp.wait()
            sends += ag_finish(rp_all, 2 * layers)
            build_masks(0)
        sends += ag_finish(g_all.at[2 * l], 2 * l)
        first_a = experts(l, 0)
        sends += ag_finish(g_all.at[2 * l + 1], 2 * l + 1)
        later = []
        first_b = experts(l, 1, lambda: later.extend(second_stage(l, 0, first_a)))
        if l == 0:
            build_masks(1)
            transpose_wo(1)
        sends += later + second_stage(l, 1, first_b)
    for hf in range(2):
        finish(layers - 1, hf)
    for cp in sends:
        cp.wait_send()
    out_ref[...] = xr_v[...].reshape(bat, d_model).astype(BF16)


def solution(mesh):
    group = mesh.shape['dp']
    chips = group // 2
    tok_axes = ('replica', 'dp')
    in_specs = (
        P(tok_axes, None), P(tok_axes), P(None, tok_axes, None, None),
        P(None, None, None), P(None, None, None),
        P(None, tok_axes, None), P(None, tok_axes, None), P(None, tok_axes, None),
        P(None, 'dp', None, None), P(None, 'dp', None, None), P(None, 'dp', None, None),
        P(None, None, 'dp'), P(None, None, 'dp'), P(None, 'dp', None),
    )

    def device_step(x, lengths, cache, w_q, w_o, expert_ids, slots, route_w, w1_exp, w3_exp, w2_exp, w1_sh, w3_sh, w2_sh):
        bat, d_model = x.shape
        layers, _, seq_len, kv_dim = cache.shape
        n_exp, ff = w1_exp.shape[1], w1_exp.shape[3]
        top_k = expert_ids.shape[2]
        heads = w_q.shape[2] // kv_dim
        assert max(1, (2 * bat * top_k) // (n_exp * group)) == 1 and layers == 2 and chips == 8
        swap = lambda a: jnp.swapaxes(a, -1, -2)
        args = (lengths, x, swap(cache), w_q, swap(w_o), swap(expert_ids), swap(slots), swap(route_w),
                w1_exp, w3_exp, swap(w2_exp), swap(w1_sh), swap(w3_sh), w2_sh)
        vm = lambda a: pltpu.VMEM(a.shape, a.dtype)
        dma = pltpu.SemaphoreType.DMA
        phs = 2 * layers
        hb = bat // 2
        toks = group * hb
        slots_n = n_exp * group
        scratch = [vm(a) for a in args[1:]] + [
            pltpu.VMEM((group, 2, 2 * layers * top_k, toks), F32),
            pltpu.VMEM((layers, 2, slots_n, toks), BF16),
            pltpu.VMEM((layers, 2, 3, toks, slots_n), BF16),
            pltpu.VMEM((phs, group, hb, d_model), BF16),
            pltpu.VMEM((phs, chips, hb, d_model), F32),
            pltpu.VMEM((phs, chips, hb, d_model), F32),
            pltpu.VMEM((phs, chips, hb, d_model), F32),
            pltpu.VMEM((phs, chips, hb, d_model), F32),
            pltpu.VMEM((phs, chips, hb, d_model), F32),
            pltpu.VMEM((2, hb, d_model), F32),
            pltpu.VMEM((layers, heads * LATENT, d_model), BF16),
            pltpu.VMEM((-(-kv_dim // 128), heads * hb, 128), F32),
            pltpu.VMEM((heads * hb, seq_len), F32),
            pltpu.VMEM((LATENT // 128, heads * hb, 128), F32),
            pltpu.VMEM((slots_n, d_model), BF16),
            pltpu.VMEM((slots_n, d_model), BF16),
            pltpu.VMEM((toks, d_model), F32),
            dma((17,)), dma((layers, bat // 4)),
            dma((phs + 1, chips)), dma((phs + 1, group)), dma((phs + 1, chips)),
            dma((phs,)), dma((phs,)), dma((phs, chips)), dma((phs, chips)),
        ]
        return pl.pallas_call(
            functools.partial(step_kernel, chips),
            out_shape=jax.ShapeDtypeStruct(x.shape, x.dtype),
            in_specs=[pl.BlockSpec(memory_space=pltpu.SMEM)] + [pl.BlockSpec(memory_space=pl.ANY)] * (len(args) - 1),
            out_specs=pl.BlockSpec(memory_space=pltpu.VMEM),
            scratch_shapes=scratch,
            compiler_params=pltpu.CompilerParams(collective_id=0, has_side_effects=True, vmem_limit_bytes=67043328),
        )(*args)

    return jax.shard_map(device_step, mesh=mesh, in_specs=in_specs, out_specs=P(tok_axes, None), check_vma=False)
```

```python
import functools

import jax
import jax.numpy as jnp
from jax import lax
from jax.experimental import pallas as pl
from jax.experimental.pallas import tpu as pltpu
from jax.sharding import PartitionSpec as P

NORM_EPS = 1e-6
ATT_SCALE = 1.0 / (192.0 ** 0.5)
LATENT = 512
MESH = pl.DeviceIdType.MESH
F32 = jnp.float32
BF16 = jnp.bfloat16


def rms_norm(vals32):
    return vals32 * lax.rsqrt(jnp.mean(vals32 * vals32, axis=-1, keepdims=True) + NORM_EPS)


def dot(lhs, rhs):
    return jnp.dot(lhs, rhs, preferred_element_type=F32)


def dot_t(lhs, rhs):
    return lax.dot_general(lhs, rhs, (((1,), (1,)), ((), ())), preferred_element_type=F32)


def step_kernel(chips, len_hbm, x_hbm, cache_hbm, wq_hbm, wo_hbm, ids_hbm, slots_hbm, rw_hbm, w1_hbm, w3_hbm, w2_hbm,
                w1s_hbm, w3s_hbm, w2s_hbm, out_ref,
                len_ref, x_v, cache_v, wq_v, wo_v, ids_v, slots_v, rw_v, w1_v, w3_v, w2_v, w1s_v, w3s_v, w2s_v,
                rp_all, oh_v, owt_v, g_all, p_buf, own_buf, r1_buf, s_buf, r2_buf,
                xr_v, wot_v, q_v, sc_v, o_v, xg_v, u_v, sh_v,
                loc_sem, cache_sem, ag_send, ag_recv, rs1_send, rs1_recv, rs2_send, rs2_recv):
    layers, bat, kv_dim, seq_len = cache_v.shape
    d_model = x_v.shape[1]
    heads = wq_v.shape[2] // kv_dim
    n_exp = w1_v.shape[1]
    ff = w1_v.shape[3]
    top_k = ids_v.shape[1]
    group = 2 * chips
    hb = bat // 2
    rows = heads * hb
    toks = group * hb
    half = chips * hb
    quad = 4

    me = lax.axis_index('dp')
    chip = me // 2
    core = me % 2
    other = 1 - core
    q_me = core * chips + chip
    partner = me + 1 - 2 * core

    far_first = (4, 3, 5, 2, 6, 1, 7)
    near_first = (1, 7, 2, 6, 3, 5, 4)

    def chip_at(delta):
        return lax.rem(chip + delta, chips)

    def load(src, dst, idx):
        return pltpu.make_async_copy(src, dst, loc_sem.at[idx])

    small = [load(x_hbm, x_v, 0), load(ids_hbm, ids_v, 1), load(slots_hbm, slots_v, 2), load(rw_hbm, rw_v, 3),
             load(w1s_hbm, w1s_v, 4), load(w3s_hbm, w3s_v, 5), load(w2s_hbm, w2s_v, 6)]
    wq_cp = [load(wq_hbm.at[l], wq_v.at[l], 7 + l) for l in range(layers)]
    wo_cp = [load(wo_hbm.at[l], wo_v.at[l], 9 + l) for l in range(layers)]
    w3_cp = [load(w3_hbm.at[l], w3_v.at[l], 11 + l) for l in range(layers)]
    w1_cp = [load(w1_hbm.at[l], w1_v.at[l], 13 + l) for l in range(layers)]
    w2_cp = [load(w2_hbm.at[l], w2_v.at[l], 15 + l) for l in range(layers)]
    cache_cp = [[pltpu.make_async_copy(cache_hbm.at[l, pl.ds(quad * c, quad)], cache_v.at[l, pl.ds(quad * c, quad)],
                                       cache_sem.at[l, c]) for c in range(bat // quad)] for l in range(layers)]

    small[0].start()
    wq_cp[0].start()
    len_cp = pltpu.make_async_copy(len_hbm, len_ref, loc_sem.at[17])
    for cp in small[1:4]:
        cp.start()
    cache_cp[0][0].start()
    wo_cp[0].start()
    for cp in cache_cp[0][1:]:
        cp.start()
    len_cp.start()
    for cp in small[4:]:
        cp.start()

    barrier = pltpu.get_barrier_semaphore()
    for delta in far_first:
        pl.semaphore_signal(barrier, inc=1, device_id={'dp': 2 * chip_at(delta) + core}, device_id_type=MESH)
    pl.semaphore_signal(barrier, inc=1, device_id={'dp': partner}, device_id_type=MESH)

    def remote(src, dst, send, recv, dev):
        return pltpu.make_async_remote_copy(src_ref=src, dst_ref=dst, send_sem=send, recv_sem=recv,
                                            device_id={'dp': dev}, device_id_type=MESH)

    def ag_start(buf, ph):
        mine = buf.at[q_me]
        cps = [remote(mine, mine, ag_send.at[ph, i], ag_recv.at[ph, chip], 2 * chip_at(delta) + core)
               for i, delta in enumerate(far_first)]
        for cp in cps:
            cp.start()
        return cps

    def ag_finish(buf, ph):
        for i, delta in enumerate(near_first):
            src = chip_at(chips - delta)
            q = core * chips + src
            remote(buf.at[q], buf.at[q], ag_send.at[ph, 0], ag_recv.at[ph, src], partner).wait_recv()
        mine = buf.at[pl.ds(core * chips, chips)]
        theirs = buf.at[pl.ds(other * chips, chips)]
        cp = remote(mine, mine, ag_send.at[ph, chips - 1], ag_recv.at[ph, chips], partner)
        cp.start()
        remote(theirs, theirs, ag_send.at[ph, chips - 1], ag_recv.at[ph, chips], partner).wait_recv()
        return [cp]

    for cp in small[1:4]:
        cp.wait()
    pieces = [jnp.where(slots_v[l] >= 0, ids_v[l] + 1, 0).astype(F32) for l in range(layers)]
    pieces += [rw_v[l] for l in range(layers)]
    pieces.append(jnp.zeros((top_k, toks - 2 * layers * bat), F32))
    rp_all[q_me] = jnp.concatenate(pieces, axis=1)

    pl.semaphore_wait(barrier, chips)
    sends = ag_start(rp_all, 2 * layers)

    small[0].wait()
    xr_v[...] = x_v[...].astype(F32).reshape(2, hb, d_model)

    def transpose_wo(l):
        wo_cp[l].wait()
        for k in range(heads * LATENT // 128):
            wot_v[l, 128 * k:128 * (k + 1), :] = wo_v[l, :, 128 * k:128 * (k + 1)].T

    def attention(l, hf):
        hidden = rms_norm(xr_v[hf]).astype(BF16)
        if hf == 0:
            wq_cp[l].wait()
        q = dot(hidden, wq_v[l])
        for hd in range(heads):
            part = q if hd == 0 else pltpu.roll(q, heads * kv_dim - hd * kv_dim, 1)
            for k in range(q_v.shape[0]):
                q_v[k, pl.ds(hd, hb, stride=heads), :] = part[:, 128 * k:128 * (k + 1)]
        for c in range(2):
            cache_cp[l][2 * hf + c].wait()
            for i in range(quad):
                b = quad * c + i
                qb = jnp.concatenate([q_v[k, heads * b:heads * (b + 1), :] for k in range(q_v.shape[0])], axis=1)
                qb = qb[:, :kv_dim].astype(BF16)
                sc_v[heads * b:heads * (b + 1), :] = dot(qb, cache_v[l, hf * hb + b])
            if l == 0 and hf == 0 and c == 0:
                transpose_wo(0)
        if l == 0 and hf == 0:
            for cps in (w3_cp, w1_cp, w2_cp):
                cps[0].start()
        row_tok = lax.broadcasted_iota(jnp.int32, (rows, 1), 0) // heads
        if l == 0 and hf == 0:
            len_cp.wait()
        lens = jnp.zeros((rows, 1), jnp.int32)
        for b in range(hb):
            lens = jnp.where(row_tok == b, len_ref[hf * hb + b], lens)
        valid = lax.broadcasted_iota(jnp.int32, (rows, seq_len), 1) < lens
        scores = jnp.where(valid, sc_v[...] * ATT_SCALE, -jnp.inf)
        top = jnp.max(scores, axis=1, keepdims=True)
        ex = jnp.exp(scores - top)
        probs = ex / jnp.sum(ex, axis=1, keepdims=True)
        sc_v[...] = probs
        for b in range(hb):
            pb = sc_v[heads * b:heads * (b + 1), :].astype(BF16)
            ob = dot_t(pb, cache_v[l, hf * hb + b, 0:LATENT, :])
            for k in range(o_v.shape[0]):
                o_v[k, heads * b:heads * (b + 1), :] = ob[:, 128 * k:128 * (k + 1)]
        attn = jnp.concatenate([o_v[k, pl.ds(hd, hb, stride=heads), :] for hd in range(heads)
                                for k in range(o_v.shape[0])], axis=1).astype(BF16)
        proj = jnp.concatenate([dot(attn, wot_v[l, :, 0:256]), dot(attn, wot_v[l, :, 256:d_model])], axis=1)
        resid = (xr_v[hf] + proj).astype(BF16).astype(F32)
        xr_v[hf] = resid
        g_all[2 * l + hf, q_me] = rms_norm(resid).astype(BF16)

    def gather_field(e):
        lane_q = lax.broadcasted_iota(jnp.int32, (top_k, toks), 1) // hb
        field = jnp.zeros((top_k, toks), F32)
        for q in range(group):
            shift = (q - e) * hb % toks
            tile = rp_all[q]
            field = jnp.where(lane_q == q, tile if shift == 0 else pltpu.roll(tile, shift, 1), field)
        return field

    def build_masks(l):
        base = me * n_exp + 1
        want = (lax.broadcasted_iota(jnp.int32, (n_exp, toks), 0) + base).astype(F32)
        lane_src = lax.broadcasted_iota(jnp.int32, (group, toks), 1) // hb
        own_src = lane_src == lax.broadcasted_iota(jnp.int32, (group, toks), 0)
        for hf in range(2):
            code = gather_field(2 * l + hf)
            wval = gather_field(2 * (layers + l) + hf)
            member = jnp.zeros((n_exp, toks), F32)
            weight = jnp.zeros((n_exp, toks), F32)
            for j in range(top_k):
                hit = code[j:j + 1, :] == want
                member = jnp.where(hit, 1.0, member)
                weight = jnp.where(hit, wval[j:j + 1, :], weight)
            onehot = [jnp.where(own_src, member[n:n + 1, :], 0.0) for n in range(n_exp)]
            oh_v[l, hf] = jnp.concatenate(onehot, axis=0).astype(BF16)
            ow = jnp.concatenate([jnp.where(own_src, weight[n:n + 1, :], 0.0) for n in range(n_exp)], axis=0)
            owt = ow.T
            hi = owt.astype(BF16)
            rest = owt - hi.astype(F32)
            mid = rest.astype(BF16)
            low = (rest - mid.astype(F32)).astype(BF16)
            owt_v[l, hf, 0] = hi
            owt_v[l, hf, 1] = mid
            owt_v[l, hf, 2] = low

    unroll = 4

    def experts(l, hf, between=None):
        ph = 2 * l + hf
        g_in = g_all[ph].reshape(toks, d_model)
        xg_v[...] = dot(oh_v[l, hf], g_in).astype(BF16)
        gate = dot_t(g_in, w3s_v[l])
        up = dot_t(g_in, w1s_v[l])
        shared_h = (jax.nn.silu(gate) * up).astype(BF16)
        sh_v[...] = dot(shared_h, w2s_v[l])
        if hf == 0:
            for cps in (w3_cp, w1_cp, w2_cp):
                cps[l].wait()

        def first_layer(pair):
            hid = []
            for e in range(2):
                n = 2 * pair + e
                start = pl.multiple_of(n * group, group)
                xin = xg_v[pl.ds(start, group), :]
                w31 = jnp.concatenate([w3_v[l, n], w1_v[l, n]], axis=1)
                both = dot(xin, w31)
                hid.append((jax.nn.silu(both[:, :ff]) * both[:, ff:]).astype(BF16))
            zero = jnp.zeros((group, ff), BF16)
            return jnp.concatenate([jnp.concatenate([hid[0], zero], axis=1),
                                    jnp.concatenate([zero, hid[1]], axis=1)], axis=0)

        def second_layer(pair, lhs):
            w2p = jnp.concatenate([w2_v[l, 2 * pair], w2_v[l, 2 * pair + 1]], axis=1)
            start = pl.multiple_of(pair * 2 * group, 2 * group)
            u_v[pl.ds(start, 2 * group), :] = dot_t(lhs, w2p).astype(BF16)

        def pair_step(i, carry):
            ready = first_layer(unroll * i)
            for jj in range(unroll):
                pair = unroll * i + jj
                coming = first_layer(pair + 1) if jj < unroll - 1 else None
                second_layer(pair, ready)
                ready = coming
            return carry

        steps = n_exp // (2 * unroll)
        lax.fori_loop(0, 1, pair_step, 0)
        if between is not None:
            between()
        lax.fori_loop(1, steps, pair_step, 0)

        def part(k):
            sel = pl.ds(pl.multiple_of(k * half, half), half)
            u_in = u_v[...]
            return sh_v[sel, :] + (dot(owt_v[l, hf, 0, sel, :], u_in) + dot(owt_v[l, hf, 1, sel, :], u_in)
                                   + dot(owt_v[l, hf, 2, sel, :], u_in))

        p_buf[ph] = part(other).reshape(chips, hb, d_model)
        first = remote(p_buf.at[ph], r1_buf.at[ph], rs1_send.at[ph], rs1_recv.at[ph], partner)
        first.start()
        own_buf[ph] = part(core).reshape(chips, hb, d_model)
        return first

    def second_stage(l, hf, first):
        ph = 2 * l + hf
        first.wait_recv()
        s_buf[ph] = own_buf[ph] + r1_buf[ph]
        cps = [first]
        for i, delta in enumerate(far_first):
            dst = chip_at(delta)
            cp = remote(s_buf.at[ph, dst], r2_buf.at[ph, chip], rs2_send.at[ph, i], rs2_recv.at[ph, chip], 2 * dst + core)
            cp.start()
            cps.append(cp)
        r2_buf[ph, chip] = s_buf[ph, chip]
        return cps

    def finish(l, hf):
        ph = 2 * l + hf
        for i, delta in enumerate(near_first):
            src = chip_at(chips - delta)
            remote(s_buf.at[ph, src], r2_buf.at[ph, src], rs2_send.at[ph, 0], rs2_recv.at[ph, src], partner).wait_recv()
        tot = r2_buf[ph, 0]
        for j in range(1, chips):
            tot = tot + r2_buf[ph, j]
        xr_v[hf] = (xr_v[hf] + tot).astype(BF16).astype(F32)

    for l in range(layers):
        for hf in range(2):
            if l > 0:
                finish(l - 1, hf)
            attention(l, hf)
            sends += ag_start(g_all.at[2 * l + hf], 2 * l + hf)
        if l == 0:
            for cp in small[4:]:
                cp.wait()
            sends += ag_finish(rp_all, 2 * layers)
            build_masks(0)
        sends += ag_finish(g_all.at[2 * l], 2 * l)
        if l == 0:
            wq_cp[1].start()
            for cp in cache_cp[1]:
                cp.start()
            wo_cp[1].start()
        first_a = experts(l, 0)
        sends += ag_finish(g_all.at[2 * l + 1], 2 * l + 1)
        later = []
        if l == 0:
            for cp_list in (w3_cp, w1_cp, w2_cp):
                cp_list[1].start()
        first_b = experts(l, 1, lambda: later.extend(second_stage(l, 0, first_a)))
        if l == 0:
            build_masks(1)
            transpose_wo(1)
        sends += later + second_stage(l, 1, first_b)
    for hf in range(2):
        finish(layers - 1, hf)
    for cp in sends:
        cp.wait_send()
    out_ref[...] = xr_v[...].reshape(bat, d_model).astype(BF16)


def solution(mesh):
    group = mesh.shape['dp']
    chips = group // 2
    tok_axes = ('replica', 'dp')
    in_specs = (
        P(tok_axes, None), P(tok_axes), P(None, tok_axes, None, None),
        P(None, None, None), P(None, None, None),
        P(None, tok_axes, None), P(None, tok_axes, None), P(None, tok_axes, None),
        P(None, 'dp', None, None), P(None, 'dp', None, None), P(None, 'dp', None, None),
        P(None, None, 'dp'), P(None, None, 'dp'), P(None, 'dp', None),
    )

    def device_step(x, lengths, cache, w_q, w_o, expert_ids, slots, route_w, w1_exp, w3_exp, w2_exp, w1_sh, w3_sh, w2_sh):
        bat, d_model = x.shape
        layers, _, seq_len, kv_dim = cache.shape
        n_exp, ff = w1_exp.shape[1], w1_exp.shape[3]
        top_k = expert_ids.shape[2]
        heads = w_q.shape[2] // kv_dim
        assert max(1, (2 * bat * top_k) // (n_exp * group)) == 1 and layers == 2 and chips == 8
        swap = lambda a: jnp.swapaxes(a, -1, -2)
        args = (lengths, x, swap(cache), w_q, swap(w_o), swap(expert_ids), swap(slots), swap(route_w),
                w1_exp, w3_exp, swap(w2_exp), swap(w1_sh), swap(w3_sh), w2_sh)
        vm = lambda a: pltpu.VMEM(a.shape, a.dtype)
        dma = pltpu.SemaphoreType.DMA
        phs = 2 * layers
        hb = bat // 2
        toks = group * hb
        slots_n = n_exp * group
        scratch = [pltpu.SMEM(lengths.shape, lengths.dtype)] + [vm(a) for a in args[1:]] + [
            pltpu.VMEM((group, top_k, toks), F32),
            pltpu.VMEM((layers, 2, slots_n, toks), BF16),
            pltpu.VMEM((layers, 2, 3, toks, slots_n), BF16),
            pltpu.VMEM((phs, group, hb, d_model), BF16),
            pltpu.VMEM((phs, chips, hb, d_model), F32),
            pltpu.VMEM((phs, chips, hb, d_model), F32),
            pltpu.VMEM((phs, chips, hb, d_model), F32),
            pltpu.VMEM((phs, chips, hb, d_model), F32),
            pltpu.VMEM((phs, chips, hb, d_model), F32),
            pltpu.VMEM((2, hb, d_model), F32),
            pltpu.VMEM((layers, heads * LATENT, d_model), BF16),
            pltpu.VMEM((-(-kv_dim // 128), heads * hb, 128), F32),
            pltpu.VMEM((heads * hb, seq_len), F32),
            pltpu.VMEM((LATENT // 128, heads * hb, 128), F32),
            pltpu.VMEM((slots_n, d_model), BF16),
            pltpu.VMEM((slots_n, d_model), BF16),
            pltpu.VMEM((toks, d_model), F32),
            dma((18,)), dma((layers, bat // 4)),
            dma((phs + 1, chips)), dma((phs + 1, chips + 1)),
            dma((phs,)), dma((phs,)), dma((phs, chips)), dma((phs, chips)),
        ]
        return pl.pallas_call(
            functools.partial(step_kernel, chips),
            out_shape=jax.ShapeDtypeStruct(x.shape, x.dtype),
            in_specs=[pl.BlockSpec(memory_space=pl.ANY)] * len(args),
            out_specs=pl.BlockSpec(memory_space=pltpu.VMEM),
            scratch_shapes=scratch,
            compiler_params=pltpu.CompilerParams(collective_id=0, has_side_effects=True, vmem_limit_bytes=67043328),
        )(*args)

    return jax.shard_map(device_step, mesh=mesh, in_specs=in_specs, out_specs=P(tok_axes, None), check_vma=False)
```

```python
import functools

import jax
import jax.numpy as jnp
from jax import lax
from jax.experimental import pallas as pl
from jax.experimental.pallas import tpu as pltpu
from jax.sharding import PartitionSpec as P

NORM_EPS = 1e-6
ATT_SCALE = 1.0 / (192.0 ** 0.5)
LATENT = 512
MESH = pl.DeviceIdType.MESH
F32 = jnp.float32
BF16 = jnp.bfloat16


def rms_norm(vals32):
    return vals32 * lax.rsqrt(jnp.mean(vals32 * vals32, axis=-1, keepdims=True) + NORM_EPS)


def dot(lhs, rhs):
    return jnp.dot(lhs, rhs, preferred_element_type=F32)


def dot_t(lhs, rhs):
    return lax.dot_general(lhs, rhs, (((1,), (1,)), ((), ())), preferred_element_type=F32)


def step_kernel(chips, len_hbm, x_hbm, cache_hbm, wq_hbm, wo_hbm, ids_hbm, slots_hbm, rw_hbm, w1_hbm, w3_hbm, w2_hbm,
                w1s_hbm, w3s_hbm, w2s_hbm, out_ref,
                len_ref, x_v, cache_v, wq_v, wo_v, ids_v, slots_v, rw_v, w1_v, w3_v, w2_v, w1s_v, w3s_v, w2s_v,
                rp_all, oh_v, owt_v, g_all, p_buf, own_buf, r1_buf, s_buf, r2_buf,
                xr_v, wot_v, q_v, sc_v, o_v, xg_v, u_v, sh_v,
                loc_sem, cache_sem, ag_send, ag_recv, rs1_send, rs1_recv, rs2_send, rs2_recv):
    layers, bat, kv_dim, seq_len = cache_v.shape
    d_model = x_v.shape[1]
    heads = wq_v.shape[2] // kv_dim
    n_exp = w1_v.shape[1]
    ff = w1_v.shape[3]
    top_k = ids_v.shape[1]
    group = 2 * chips
    hb = bat // 2
    rows = heads * hb
    toks = group * hb
    half = chips * hb
    quad = 4

    me = lax.axis_index('dp')
    chip = me // 2
    core = me % 2
    other = 1 - core
    q_me = core * chips + chip
    partner = me + 1 - 2 * core

    far_first = (4, 3, 5, 2, 6, 1, 7)
    near_first = (1, 7, 2, 6, 3, 5, 4)

    def chip_at(delta):
        return lax.rem(chip + delta, chips)

    def load(src, dst, idx):
        return pltpu.make_async_copy(src, dst, loc_sem.at[idx])

    small = [load(x_hbm, x_v, 0), load(ids_hbm, ids_v, 1), load(slots_hbm, slots_v, 2), load(rw_hbm, rw_v, 3),
             load(w1s_hbm, w1s_v, 4), load(w3s_hbm, w3s_v, 5), load(w2s_hbm, w2s_v, 6)]
    wq_cp = [load(wq_hbm.at[l], wq_v.at[l], 7 + l) for l in range(layers)]
    wo_cp = [load(wo_hbm.at[l], wo_v.at[l], 9 + l) for l in range(layers)]
    w3_cp = [load(w3_hbm.at[l], w3_v.at[l], 11 + l) for l in range(layers)]
    w1_cp = [load(w1_hbm.at[l], w1_v.at[l], 13 + l) for l in range(layers)]
    w2_cp = [load(w2_hbm.at[l], w2_v.at[l], 15 + l) for l in range(layers)]
    cache_cp = [[pltpu.make_async_copy(cache_hbm.at[l, pl.ds(quad * c, quad)], cache_v.at[l, pl.ds(quad * c, quad)],
                                       cache_sem.at[l, c]) for c in range(bat // quad)] for l in range(layers)]

    small[0].start()
    wq_cp[0].start()
    len_cp = pltpu.make_async_copy(len_hbm, len_ref, loc_sem.at[17])
    for cp in small[1:4]:
        cp.start()
    cache_cp[0][0].start()
    wo_cp[0].start()
    for cp in cache_cp[0][1:]:
        cp.start()
    len_cp.start()
    for cp in small[4:]:
        cp.start()

    barrier = pltpu.get_barrier_semaphore()
    for delta in far_first:
        pl.semaphore_signal(barrier, inc=1, device_id={'dp': 2 * chip_at(delta) + core}, device_id_type=MESH)
    pl.semaphore_signal(barrier, inc=1, device_id={'dp': partner}, device_id_type=MESH)

    def remote(src, dst, send, recv, dev):
        return pltpu.make_async_remote_copy(src_ref=src, dst_ref=dst, send_sem=send, recv_sem=recv,
                                            device_id={'dp': dev}, device_id_type=MESH)

    def ag_start(buf, ph):
        mine = buf.at[q_me]
        cps = [remote(mine, mine, ag_send.at[ph, i], ag_recv.at[ph, chip], 2 * chip_at(delta) + core)
               for i, delta in enumerate(far_first)]
        for cp in cps:
            cp.start()
        return cps

    def ag_finish(buf, ph):
        for i, delta in enumerate(near_first):
            src = chip_at(chips - delta)
            q = core * chips + src
            remote(buf.at[q], buf.at[q], ag_send.at[ph, 0], ag_recv.at[ph, src], partner).wait_recv()
        mine = buf.at[pl.ds(core * chips, chips)]
        theirs = buf.at[pl.ds(other * chips, chips)]
        cp = remote(mine, mine, ag_send.at[ph, chips - 1], ag_recv.at[ph, chips], partner)
        cp.start()
        remote(theirs, theirs, ag_send.at[ph, chips - 1], ag_recv.at[ph, chips], partner).wait_recv()
        return [cp]

    for cp in small[1:4]:
        cp.wait()
    pieces = [jnp.where(slots_v[l] >= 0, ids_v[l] + 1, 0).astype(F32) for l in range(layers)]
    pieces += [rw_v[l] for l in range(layers)]
    pieces.append(jnp.zeros((top_k, toks - 2 * layers * bat), F32))
    rp_all[q_me] = jnp.concatenate(pieces, axis=1)

    pl.semaphore_wait(barrier, chips)
    sends = ag_start(rp_all, 2 * layers)

    small[0].wait()
    xr_v[...] = x_v[...].astype(F32).reshape(2, hb, d_model)

    def transpose_wo(l):
        wo_cp[l].wait()
        for k in range(heads * LATENT // 128):
            wot_v[128 * k:128 * (k + 1), :] = wo_v[l, :, 128 * k:128 * (k + 1)].T

    def transpose_cache(hf):
        for c in range(2):
            cache_cp[1][2 * hf + c].wait()
            for i in range(quad):
                b = hf * hb + quad * c + i
                cache_v[0, b, 0:LATENT, :] = cache_v[1, b, 0:LATENT, :].T

    def attention(l, hf):
        hidden = rms_norm(xr_v[hf]).astype(BF16)
        if hf == 0:
            wq_cp[l].wait()
        q = dot(hidden, wq_v[l])
        for hd in range(heads):
            part = q if hd == 0 else pltpu.roll(q, heads * kv_dim - hd * kv_dim, 1)
            for k in range(q_v.shape[0]):
                q_v[k, pl.ds(hd, hb, stride=heads), :] = part[:, 128 * k:128 * (k + 1)]
        for c in range(2):
            if l == 0:
                cache_cp[l][2 * hf + c].wait()
            for i in range(quad):
                b = quad * c + i
                qb = jnp.concatenate([q_v[k, heads * b:heads * (b + 1), :] for k in range(q_v.shape[0])], axis=1)
                qb = qb[:, :kv_dim].astype(BF16)
                sc_v[heads * b:heads * (b + 1), :] = dot(qb, cache_v[l, hf * hb + b])
            if l == 0 and hf == 0 and c == 0:
                transpose_wo(0)
        if l == 0 and hf == 0:
            for cps in (w3_cp, w1_cp, w2_cp):
                cps[0].start()
        row_tok = lax.broadcasted_iota(jnp.int32, (rows, 1), 0) // heads
        if l == 0 and hf == 0:
            len_cp.wait()
        lens = jnp.zeros((rows, 1), jnp.int32)
        for b in range(hb):
            lens = jnp.where(row_tok == b, len_ref[hf * hb + b], lens)
        valid = lax.broadcasted_iota(jnp.int32, (rows, seq_len), 1) < lens
        scores = jnp.where(valid, sc_v[...] * ATT_SCALE, -jnp.inf)
        top = jnp.max(scores, axis=1, keepdims=True)
        ex = jnp.exp(scores - top)
        probs = ex / jnp.sum(ex, axis=1, keepdims=True)
        sc_v[...] = probs
        for b in range(hb):
            pb = sc_v[heads * b:heads * (b + 1), :].astype(BF16)
            if l == 0:
                ob = dot_t(pb, cache_v[0, hf * hb + b, 0:LATENT, :])
            else:
                ob = dot(pb, cache_v[0, hf * hb + b, 0:LATENT, :])
            for k in range(o_v.shape[0]):
                o_v[k, heads * b:heads * (b + 1), :] = ob[:, 128 * k:128 * (k + 1)]
        attn = jnp.concatenate([o_v[k, pl.ds(hd, hb, stride=heads), :] for hd in range(heads)
                                for k in range(o_v.shape[0])], axis=1).astype(BF16)
        proj = jnp.concatenate([dot(attn, wot_v[:, 0:256]), dot(attn, wot_v[:, 256:d_model])], axis=1)
        resid = (xr_v[hf] + proj).astype(BF16).astype(F32)
        xr_v[hf] = resid
        g_all[2 * l + hf, q_me] = rms_norm(resid).astype(BF16)

    def gather_field(e):
        lane_q = lax.broadcasted_iota(jnp.int32, (top_k, toks), 1) // hb
        field = jnp.zeros((top_k, toks), F32)
        for q in range(group):
            shift = (q - e) * hb % toks
            tile = rp_all[q]
            field = jnp.where(lane_q == q, tile if shift == 0 else pltpu.roll(tile, shift, 1), field)
        return field

    def build_masks(l):
        base = me * n_exp + 1
        want = (lax.broadcasted_iota(jnp.int32, (n_exp, toks), 0) + base).astype(F32)
        lane_src = lax.broadcasted_iota(jnp.int32, (group, toks), 1) // hb
        own_src = lane_src == lax.broadcasted_iota(jnp.int32, (group, toks), 0)
        for hf in range(2):
            code = gather_field(2 * l + hf)
            wval = gather_field(2 * (layers + l) + hf)
            member = jnp.zeros((n_exp, toks), F32)
            weight = jnp.zeros((n_exp, toks), F32)
            for j in range(top_k):
                hit = code[j:j + 1, :] == want
                member = jnp.where(hit, 1.0, member)
                weight = jnp.where(hit, wval[j:j + 1, :], weight)
            onehot = [jnp.where(own_src, member[n:n + 1, :], 0.0) for n in range(n_exp)]
            oh_v[l, hf] = jnp.concatenate(onehot, axis=0).astype(BF16)
            ow = jnp.concatenate([jnp.where(own_src, weight[n:n + 1, :], 0.0) for n in range(n_exp)], axis=0)
            owt = ow.T
            hi = owt.astype(BF16)
            rest = owt - hi.astype(F32)
            mid = rest.astype(BF16)
            low = (rest - mid.astype(F32)).astype(BF16)
            for k in range(2):
                for i, term in enumerate((hi, mid, low)):
                    owt_v[l, hf, k, i * half:(i + 1) * half, :] = term[k * half:(k + 1) * half, :]

    def experts(l, hf, between=None):
        ph = 2 * l + hf
        g_in = g_all[ph].reshape(toks, d_model)
        xg_v[...] = dot(oh_v[l, hf], g_in).astype(BF16)
        if hf == 0:
            for cps in (w3_cp, w1_cp, w2_cp):
                cps[l].wait()

        def first_layer(pair):
            hid = []
            for e in range(2):
                n = 2 * pair + e
                start = pl.multiple_of(n * group, group)
                xin = xg_v[pl.ds(start, group), :]
                w31 = jnp.concatenate([w3_v[l, n], w1_v[l, n]], axis=1)
                both = dot(xin, w31)
                hid.append((jax.nn.silu(both[:, :ff]) * both[:, ff:]).astype(BF16))
            zero = jnp.zeros((group, ff), BF16)
            return jnp.concatenate([jnp.concatenate([hid[0], zero], axis=1),
                                    jnp.concatenate([zero, hid[1]], axis=1)], axis=0)

        def second_layer(pair, lhs):
            w2p = jnp.concatenate([w2_v[l, 2 * pair], w2_v[l, 2 * pair + 1]], axis=1)
            start = pl.multiple_of(pair * 2 * group, 2 * group)
            u_v[pl.ds(start, 2 * group), :] = dot_t(lhs, w2p).astype(BF16)

        def shared_expert():
            gate = dot_t(g_in, w3s_v[l])
            up = dot_t(g_in, w1s_v[l])
            shared_h = (jax.nn.silu(gate) * up).astype(BF16)
            sh_v[...] = dot(shared_h, w2s_v[l])

        pairs = n_exp // 2
        ready = first_layer(0)
        for pair in range(pairs):
            coming = first_layer(pair + 1) if pair < pairs - 1 else None
            second_layer(pair, ready)
            ready = coming
            if pair == 2:
                shared_expert()
            if pair == 3 and between is not None:
                between()

        def part(k):
            sel = pl.ds(pl.multiple_of(k * half, half), half)
            three = dot(owt_v[l, hf, k], u_v[...])
            return sh_v[sel, :] + (three[:half] + three[half:2 * half] + three[2 * half:])

        p_buf[ph] = part(other).reshape(chips, hb, d_model)
        first = remote(p_buf.at[ph], r1_buf.at[ph], rs1_send.at[ph], rs1_recv.at[ph], partner)
        first.start()
        own_buf[ph] = part(core).reshape(chips, hb, d_model)
        return first

    def second_stage(l, hf, first):
        ph = 2 * l + hf
        first.wait_recv()
        s_buf[ph] = own_buf[ph] + r1_buf[ph]
        cps = [first]
        for i, delta in enumerate(far_first):
            dst = chip_at(delta)
            cp = remote(s_buf.at[ph, dst], r2_buf.at[ph, chip], rs2_send.at[ph, i], rs2_recv.at[ph, chip], 2 * dst + core)
            cp.start()
            cps.append(cp)
        r2_buf[ph, chip] = s_buf[ph, chip]
        return cps

    def finish(l, hf):
        ph = 2 * l + hf
        for i, delta in enumerate(near_first):
            src = chip_at(chips - delta)
            remote(s_buf.at[ph, src], r2_buf.at[ph, src], rs2_send.at[ph, 0], rs2_recv.at[ph, src], partner).wait_recv()
        tot = r2_buf[ph, 0]
        for j in range(1, chips):
            tot = tot + r2_buf[ph, j]
        xr_v[hf] = (xr_v[hf] + tot).astype(BF16).astype(F32)

    for l in range(layers):
        for hf in range(2):
            if l > 0:
                finish(l - 1, hf)
            attention(l, hf)
            sends += ag_start(g_all.at[2 * l + hf], 2 * l + hf)
            if l == 0 and hf == 0:
                for cp in cache_cp[1]:
                    cp.start()
        if l == 0:
            for cp in small[4:]:
                cp.wait()
            sends += ag_finish(rp_all, 2 * layers)
            build_masks(0)
            transpose_cache(0)
        sends += ag_finish(g_all.at[2 * l], 2 * l)
        if l == 0:
            wq_cp[1].start()
            wo_cp[1].start()
        first_a = experts(l, 0)
        sends += ag_finish(g_all.at[2 * l + 1], 2 * l + 1)
        later = []
        if l == 0:
            for cp_list in (w3_cp, w1_cp, w2_cp):
                cp_list[1].start()
        if l == 0:
            later += second_stage(l, 0, first_a)
            first_b = experts(l, 1)
            build_masks(1)
            transpose_wo(1)
        else:
            first_b = experts(l, 1, lambda: later.extend(second_stage(l, 0, first_a)))
        sends += later + second_stage(l, 1, first_b)
        if l == 0:
            transpose_cache(1)
    for hf in range(2):
        finish(layers - 1, hf)
    for cp in sends:
        cp.wait_send()
    out_ref[...] = xr_v[...].reshape(bat, d_model).astype(BF16)


def solution(mesh):
    group = mesh.shape['dp']
    chips = group // 2
    tok_axes = ('replica', 'dp')
    in_specs = (
        P(tok_axes, None), P(tok_axes), P(None, tok_axes, None, None),
        P(None, None, None), P(None, None, None),
        P(None, tok_axes, None), P(None, tok_axes, None), P(None, tok_axes, None),
        P(None, 'dp', None, None), P(None, 'dp', None, None), P(None, 'dp', None, None),
        P(None, None, 'dp'), P(None, None, 'dp'), P(None, 'dp', None),
    )

    def device_step(x, lengths, cache, w_q, w_o, expert_ids, slots, route_w, w1_exp, w3_exp, w2_exp, w1_sh, w3_sh, w2_sh):
        bat, d_model = x.shape
        layers, _, seq_len, kv_dim = cache.shape
        n_exp, ff = w1_exp.shape[1], w1_exp.shape[3]
        top_k = expert_ids.shape[2]
        heads = w_q.shape[2] // kv_dim
        assert max(1, (2 * bat * top_k) // (n_exp * group)) == 1 and layers == 2 and chips == 8
        swap = lambda a: jnp.swapaxes(a, -1, -2)
        args = (lengths, x, swap(cache), w_q, swap(w_o), swap(expert_ids), swap(slots), swap(route_w),
                w1_exp, w3_exp, swap(w2_exp), swap(w1_sh), swap(w3_sh), w2_sh)
        vm = lambda a: pltpu.VMEM(a.shape, a.dtype)
        dma = pltpu.SemaphoreType.DMA
        phs = 2 * layers
        hb = bat // 2
        toks = group * hb
        slots_n = n_exp * group
        scratch = [pltpu.SMEM(lengths.shape, lengths.dtype)] + [vm(a) for a in args[1:]] + [
            pltpu.VMEM((group, top_k, toks), F32),
            pltpu.VMEM((layers, 2, slots_n, toks), BF16),
            pltpu.VMEM((layers, 2, 2, 3 * toks // 2, slots_n), BF16),
            pltpu.VMEM((phs, group, hb, d_model), BF16),
            pltpu.VMEM((phs, chips, hb, d_model), F32),
            pltpu.VMEM((phs, chips, hb, d_model), F32),
            pltpu.VMEM((phs, chips, hb, d_model), F32),
            pltpu.VMEM((phs, chips, hb, d_model), F32),
            pltpu.VMEM((phs, chips, hb, d_model), F32),
            pltpu.VMEM((2, hb, d_model), F32),
            pltpu.VMEM((heads * LATENT, d_model), BF16),
            pltpu.VMEM((-(-kv_dim // 128), heads * hb, 128), F32),
            pltpu.VMEM((heads * hb, seq_len), F32),
            pltpu.VMEM((LATENT // 128, heads * hb, 128), F32),
            pltpu.VMEM((slots_n, d_model), BF16),
            pltpu.VMEM((slots_n, d_model), BF16),
            pltpu.VMEM((toks, d_model), F32),
            dma((18,)), dma((layers, bat // 4)),
            dma((phs + 1, chips)), dma((phs + 1, chips + 1)),
            dma((phs,)), dma((phs,)), dma((phs, chips)), dma((phs, chips)),
        ]
        return pl.pallas_call(
            functools.partial(step_kernel, chips),
            out_shape=jax.ShapeDtypeStruct(x.shape, x.dtype),
            in_specs=[pl.BlockSpec(memory_space=pltpu.HBM)] * len(args),
            out_specs=pl.BlockSpec(memory_space=pltpu.VMEM),
            scratch_shapes=scratch,
            compiler_params=pltpu.CompilerParams(collective_id=0, has_side_effects=True, vmem_limit_bytes=56000000),
        )(*[pltpu.with_memory_space_constraint(a, pltpu.HBM) for a in args])

    return jax.shard_map(device_step, mesh=mesh, in_specs=in_specs, out_specs=P(tok_axes, None), check_vma=False)
```

```python
import functools

import jax
import jax.numpy as jnp
from jax import lax
from jax.experimental import pallas as pl
from jax.experimental.pallas import tpu as pltpu
from jax.sharding import PartitionSpec as P

NORM_EPS = 1e-6
ATT_SCALE = 1.0 / (192.0 ** 0.5)
LATENT = 512
MESH = pl.DeviceIdType.MESH
F32 = jnp.float32
BF16 = jnp.bfloat16


def rms_norm(vals32):
    return vals32 * lax.rsqrt(jnp.mean(vals32 * vals32, axis=-1, keepdims=True) + NORM_EPS)


def dot(lhs, rhs):
    return jnp.dot(lhs, rhs, preferred_element_type=F32)


def dot_t(lhs, rhs):
    return lax.dot_general(lhs, rhs, (((1,), (1,)), ((), ())), preferred_element_type=F32)


def step_kernel(chips, len_hbm, x_hbm, cache_hbm, wq_hbm, wo_hbm, ids_hbm, slots_hbm, rw_hbm, w1_hbm, w3_hbm, w2_hbm,
                w1s_hbm, w3s_hbm, w2s_hbm, out_ref,
                len_ref, x_v, cache_v, wq_v, wo_v, ids_v, slots_v, rw_v, w1_v, w3_v, w2_v, w1s_v, w3s_v, w2s_v,
                rp_all, oh_v, owt_v, g_all, p_buf, own_buf, r1_buf, s_buf, r2_buf,
                xr_v, wot_v, w2t_v, q_v, sc_v, o_v, xg_v, u_v, sh_v,
                loc_sem, cache_sem, ag_send, ag_recv, rs1_send, rs1_recv, rs2_send, rs2_recv, wq_sem):
    layers, bat, kv_dim, seq_len = cache_v.shape
    d_model = x_v.shape[1]
    heads = wq_v.shape[2] // kv_dim
    n_exp = w1_v.shape[1]
    ff = w1_v.shape[3]
    top_k = ids_v.shape[1]
    group = 2 * chips
    hb = bat // 2
    rows = heads * hb
    toks = group * hb
    half = chips * hb
    quad = 4

    me = lax.axis_index('dp')
    chip = me // 2
    core = me % 2
    other = 1 - core
    q_me = core * chips + chip
    partner = me + 1 - 2 * core

    far_first = (4, 3, 5, 2, 6, 1, 7)
    near_first = (1, 7, 2, 6, 3, 5, 4)

    def chip_at(delta):
        return lax.rem(chip + delta, chips)

    def load(src, dst, idx):
        return pltpu.make_async_copy(src, dst, loc_sem.at[idx])

    small = [load(x_hbm, x_v, 0), load(ids_hbm, ids_v, 1), load(slots_hbm, slots_v, 2), load(rw_hbm, rw_v, 3),
             load(w1s_hbm, w1s_v, 4), load(w3s_hbm, w3s_v, 5), load(w2s_hbm, w2s_v, 6)]
    q_cols = wq_v.shape[2]
    q_part = q_cols // 3
    wq_cp = [[pltpu.make_async_copy(wq_hbm.at[l, :, pl.ds(q_part * c, q_part)], wq_v.at[l, :, pl.ds(q_part * c, q_part)],
                                    wq_sem.at[l, c]) for c in range(3)] for l in range(layers)]
    wo_cp = [load(wo_hbm.at[l], wo_v.at[l], 9 + l) for l in range(layers)]
    w3_cp = [load(w3_hbm.at[l], w3_v.at[l], 11 + l) for l in range(layers)]
    w1_cp = [load(w1_hbm.at[l], w1_v.at[l], 13 + l) for l in range(layers)]
    w2_cp = [load(w2_hbm.at[l], w2_v.at[l], 15 + l) for l in range(layers)]
    cache_cp = [[pltpu.make_async_copy(cache_hbm.at[l, pl.ds(quad * c, quad)], cache_v.at[l, pl.ds(quad * c, quad)],
                                       cache_sem.at[l, c]) for c in range(bat // quad)] for l in range(layers)]

    small[0].start()
    for cp in wq_cp[0]:
        cp.start()
    len_cp = pltpu.make_async_copy(len_hbm, len_ref, loc_sem.at[17])
    for cp in small[1:4]:
        cp.start()
    len_cp.start()
    for cp in cache_cp[0][:2]:
        cp.start()
    wo_cp[0].start()
    for cp in cache_cp[0][2:]:
        cp.start()
    for cp in small[4:]:
        cp.start()

    barrier = pltpu.get_barrier_semaphore()
    for delta in far_first:
        pl.semaphore_signal(barrier, inc=1, device_id={'dp': 2 * chip_at(delta) + core}, device_id_type=MESH)
    pl.semaphore_signal(barrier, inc=1, device_id={'dp': partner}, device_id_type=MESH)

    def remote(src, dst, send, recv, dev):
        return pltpu.make_async_remote_copy(src_ref=src, dst_ref=dst, send_sem=send, recv_sem=recv,
                                            device_id={'dp': dev}, device_id_type=MESH)

    def ag_start(buf, ph):
        mine = buf.at[q_me]
        cps = [remote(mine, mine, ag_send.at[ph, i], ag_recv.at[ph, chip], 2 * chip_at(delta) + core)
               for i, delta in enumerate(far_first)]
        for cp in cps:
            cp.start()
        return cps

    def ag_finish(buf, ph):
        for i, delta in enumerate(near_first):
            src = chip_at(chips - delta)
            q = core * chips + src
            remote(buf.at[q], buf.at[q], ag_send.at[ph, 0], ag_recv.at[ph, src], partner).wait_recv()
        mine = buf.at[pl.ds(core * chips, chips)]
        theirs = buf.at[pl.ds(other * chips, chips)]
        cp = remote(mine, mine, ag_send.at[ph, chips - 1], ag_recv.at[ph, chips], partner)
        cp.start()
        remote(theirs, theirs, ag_send.at[ph, chips - 1], ag_recv.at[ph, chips], partner).wait_recv()
        return [cp]

    for cp in small[1:4]:
        cp.wait()
    pieces = [jnp.where(slots_v[l] >= 0, ids_v[l] + 1, 0).astype(F32) for l in range(layers)]
    pieces += [rw_v[l] for l in range(layers)]
    pieces.append(jnp.zeros((top_k, toks - 2 * layers * bat), F32))
    rp_all[q_me] = jnp.concatenate(pieces, axis=1)

    pl.semaphore_wait(barrier, chips)
    sends = ag_start(rp_all, 2 * layers)

    small[0].wait()
    xr_v[...] = x_v[...].astype(F32).reshape(2, hb, d_model)

    def transpose_wo(l):
        wo_cp[l].wait()
        for k in range(heads * LATENT // 128):
            wot_v[128 * k:128 * (k + 1), :] = wo_v[l, :, 128 * k:128 * (k + 1)].T

    def transpose_w2(l):
        w2_cp[l].wait()
        for n in range(n_exp):
            w2t_v[ff * n:ff * (n + 1), :] = w2_v[l, n].T

    def transpose_cache(c):
        cache_cp[1][c].wait()
        for b in range(quad * c, quad * (c + 1)):
            cache_v[0, b, 0:LATENT, :] = cache_v[1, b, 0:LATENT, :].T

    def attention(l, hf):
        halves = (0, 1) if l == 0 else (hf,)
        if l > 0 or hf == 0:
            x_in = xr_v[...].reshape(bat, d_model) if l == 0 else xr_v[hf]
            hidden = rms_norm(x_in).astype(BF16)
            q = []
            if l > 0 and hf == 0:
                for cp in wq_cp[l]:
                    cp.wait()
            for c in range(3):
                if l == 0:
                    wq_cp[l][c].wait()
                q.append(dot(hidden, wq_v[l, :, q_part * c:q_part * (c + 1)]))
            q = jnp.concatenate(q, axis=1)
            for hd in range(heads):
                part = q if hd == 0 else pltpu.roll(q, q_cols - hd * kv_dim, 1)
                for i, h in enumerate(halves):
                    for k in range(q_v.shape[1]):
                        q_v[h, k, pl.ds(hd, hb, stride=heads), :] = part[hb * i:hb * (i + 1), 128 * k:128 * (k + 1)]
        if l == 0 and hf == 0:
            len_cp.wait()
        for grp in (((0,), (1,)) if l == 0 and hf == 0 else ((0, 1),)):
            first, count = heads * quad * grp[0], heads * quad * len(grp)
            seqs = range(quad * grp[0], quad * (grp[-1] + 1))
            if l == 0:
                for c in grp:
                    cache_cp[l][2 * hf + c].wait()
            for b in seqs:
                qb = jnp.concatenate([q_v[hf, k, heads * b:heads * (b + 1), :] for k in range(q_v.shape[1])], axis=1)
                qb = qb[:, :kv_dim].astype(BF16)
                sc_v[heads * b:heads * (b + 1), :] = dot(qb, cache_v[l, hf * hb + b])
            row_tok = (lax.broadcasted_iota(jnp.int32, (count, 1), 0) + first) // heads
            lens = jnp.zeros((count, 1), jnp.int32)
            for b in seqs:
                lens = jnp.where(row_tok == b, len_ref[hf * hb + b], lens)
            valid = lax.broadcasted_iota(jnp.int32, (count, seq_len), 1) < lens
            scores = jnp.where(valid, sc_v[first:first + count, :] * ATT_SCALE, -jnp.inf)
            top = jnp.max(scores, axis=1, keepdims=True)
            ex = jnp.exp(scores - top)
            sc_v[first:first + count, :] = ex / jnp.sum(ex, axis=1, keepdims=True)
            for b in seqs:
                pb = sc_v[heads * b:heads * (b + 1), :].astype(BF16)
                if l == 0:
                    ob = dot_t(pb, cache_v[0, hf * hb + b, 0:LATENT, :])
                else:
                    ob = dot(pb, cache_v[0, hf * hb + b, 0:LATENT, :])
                for k in range(o_v.shape[0]):
                    o_v[k, heads * b:heads * (b + 1), :] = ob[:, 128 * k:128 * (k + 1)]
            if l == 0 and hf == 0 and grp[0] == 0:
                for cps in (w2_cp, w3_cp, w1_cp):
                    cps[0].start()
        attn = jnp.concatenate([o_v[k, pl.ds(hd, hb, stride=heads), :] for hd in range(heads)
                                for k in range(o_v.shape[0])], axis=1).astype(BF16)
        if l == 0:
            if hf == 0:
                wo_cp[0].wait()
            proj = jnp.concatenate([dot_t(attn, wo_v[0, 0:256]), dot_t(attn, wo_v[0, 256:d_model])], axis=1)
        else:
            proj = jnp.concatenate([dot(attn, wot_v[:, 0:256]), dot(attn, wot_v[:, 256:d_model])], axis=1)
        resid = (xr_v[hf] + proj).astype(BF16).astype(F32)
        xr_v[hf] = resid
        g_all[2 * l + hf, q_me] = rms_norm(resid).astype(BF16)

    def gather_field(e):
        lane_q = lax.broadcasted_iota(jnp.int32, (top_k, toks), 1) // hb
        field = jnp.zeros((top_k, toks), F32)
        for q in range(group):
            shift = (q - e) * hb % toks
            tile = rp_all[q]
            field = jnp.where(lane_q == q, tile if shift == 0 else pltpu.roll(tile, shift, 1), field)
        return field

    def build_masks(l):
        base = me * n_exp + 1
        want = (lax.broadcasted_iota(jnp.int32, (n_exp, toks), 0) + base).astype(F32)
        lane_src = lax.broadcasted_iota(jnp.int32, (group, toks), 1) // hb
        own_src = lane_src == lax.broadcasted_iota(jnp.int32, (group, toks), 0)
        for hf in range(2):
            code = gather_field(2 * l + hf)
            wval = gather_field(2 * (layers + l) + hf)
            member = jnp.zeros((n_exp, toks), F32)
            weight = jnp.zeros((n_exp, toks), F32)
            for j in range(top_k):
                hit = code[j:j + 1, :] == want
                member = jnp.where(hit, 1.0, member)
                weight = jnp.where(hit, wval[j:j + 1, :], weight)
            onehot = [jnp.where(own_src, member[n:n + 1, :], 0.0) for n in range(n_exp)]
            oh_v[l, hf] = jnp.concatenate(onehot, axis=0).astype(BF16)
            ow = jnp.concatenate([jnp.where(own_src, weight[n:n + 1, :], 0.0) for n in range(n_exp)], axis=0)
            owt = ow.T
            hi = owt.astype(BF16)
            rest = owt - hi.astype(F32)
            mid = rest.astype(BF16)
            low = (rest - mid.astype(F32)).astype(BF16)
            for k in range(2):
                for i, term in enumerate((hi, mid, low)):
                    owt_v[l, hf, k, i * half:(i + 1) * half, :] = term[k * half:(k + 1) * half, :]

    def experts(l, hf, between=None):
        ph = 2 * l + hf
        g_in = g_all[ph].reshape(toks, d_model)
        xg_v[...] = dot(oh_v[l, hf], g_in).astype(BF16)
        if hf == 0:
            for cps in (w3_cp, w1_cp):
                cps[l].wait()

        def first_layer(pair):
            hid = []
            for e in range(2):
                n = 2 * pair + e
                xin = xg_v[group * n:group * (n + 1), :]
                w31 = jnp.concatenate([w3_v[l, n], w1_v[l, n]], axis=1)
                both = dot(xin, w31)
                hid.append((jax.nn.silu(both[:, :ff]) * both[:, ff:]).astype(BF16))
            zero = jnp.zeros((group, ff), BF16)
            return jnp.concatenate([jnp.concatenate([hid[0], zero], axis=1),
                                    jnp.concatenate([zero, hid[1]], axis=1)], axis=0)

        def second_layer(pair, lhs):
            u_v[2 * group * pair:2 * group * (pair + 1), :] = dot(lhs, w2t_v[2 * ff * pair:2 * ff * (pair + 1), :]).astype(BF16)

        def shared_expert():
            gate = dot_t(g_in, w3s_v[l])
            up = dot_t(g_in, w1s_v[l])
            shared_h = (jax.nn.silu(gate) * up).astype(BF16)
            sh_v[...] = dot(shared_h, w2s_v[l])

        pairs = n_exp // 2
        ready = first_layer(0)
        for pair in range(pairs):
            coming = first_layer(pair + 1) if pair < pairs - 1 else None
            second_layer(pair, ready)
            ready = coming
            if pair == 2:
                shared_expert()
            if pair == 3 and between is not None:
                between()

        def part(k):
            sel = pl.ds(pl.multiple_of(k * half, half), half)
            three = dot(owt_v[l, hf, k], u_v[...])
            return sh_v[sel, :] + (three[:half] + three[half:2 * half] + three[2 * half:])

        p_buf[ph] = part(other).reshape(chips, hb, d_model)
        first = remote(p_buf.at[ph], r1_buf.at[ph], rs1_send.at[ph], rs1_recv.at[ph], partner)
        first.start()
        own_buf[ph] = part(core).reshape(chips, hb, d_model)
        return first

    def second_stage(l, hf, first):
        ph = 2 * l + hf
        first.wait_recv()
        s_buf[ph] = own_buf[ph] + r1_buf[ph]
        cps = [first]
        for i, delta in enumerate(far_first):
            dst = chip_at(delta)
            cp = remote(s_buf.at[ph, dst], r2_buf.at[ph, chip], rs2_send.at[ph, i], rs2_recv.at[ph, chip], 2 * dst + core)
            cp.start()
            cps.append(cp)
        r2_buf[ph, chip] = s_buf[ph, chip]
        return cps

    def finish(l, hf):
        ph = 2 * l + hf
        for i, delta in enumerate(near_first):
            src = chip_at(chips - delta)
            remote(s_buf.at[ph, src], r2_buf.at[ph, src], rs2_send.at[ph, 0], rs2_recv.at[ph, src], partner).wait_recv()
        tot = r2_buf[ph, 0]
        for j in range(1, chips):
            tot = tot + r2_buf[ph, j]
        xr_v[hf] = (xr_v[hf] + tot).astype(BF16).astype(F32)

    attention(0, 0)
    sends += ag_start(g_all.at[0], 0)
    attention(0, 1)
    sends += ag_start(g_all.at[1], 1)
    for cp in cache_cp[1]:
        cp.start()
    for cp in small[4:]:
        cp.wait()
    sends += ag_finish(rp_all, 2 * layers)
    build_masks(0)
    transpose_w2(0)
    sends += ag_finish(g_all.at[0], 0)
    for cp in wq_cp[1] + [wo_cp[1]]:
        cp.start()
    later = []
    first_a = experts(0, 0)
    sends += ag_finish(g_all.at[1], 1)
    for cp_list in (w3_cp, w1_cp, w2_cp):
        cp_list[1].start()
    first_b = experts(0, 1, lambda: later.extend(second_stage(0, 0, first_a)))
    build_masks(1)
    transpose_cache(0)
    later += second_stage(0, 1, first_b)
    for c in range(1, bat // quad):
        transpose_cache(c)
    transpose_wo(1)
    finish(0, 0)
    attention(1, 0)
    sends += ag_start(g_all.at[2], 2)
    finish(0, 1)
    attention(1, 1)
    sends += ag_start(g_all.at[3], 3)
    transpose_w2(1)
    sends += ag_finish(g_all.at[2], 2)
    first_a = experts(1, 0)
    sends += ag_finish(g_all.at[3], 3)
    first_b = experts(1, 1, lambda: later.extend(second_stage(1, 0, first_a)))
    sends += later + second_stage(1, 1, first_b)
    for hf in range(2):
        finish(layers - 1, hf)
    for cp in sends:
        cp.wait_send()
    out_ref[...] = xr_v[...].reshape(bat, d_model).astype(BF16)


def solution(mesh):
    group = mesh.shape['dp']
    chips = group // 2
    tok_axes = ('replica', 'dp')
    in_specs = (
        P(tok_axes, None), P(tok_axes), P(None, tok_axes, None, None),
        P(None, None, None), P(None, None, None),
        P(None, tok_axes, None), P(None, tok_axes, None), P(None, tok_axes, None),
        P(None, 'dp', None, None), P(None, 'dp', None, None), P(None, 'dp', None, None),
        P(None, None, 'dp'), P(None, None, 'dp'), P(None, 'dp', None),
    )

    def device_step(x, lengths, cache, w_q, w_o, expert_ids, slots, route_w, w1_exp, w3_exp, w2_exp, w1_sh, w3_sh, w2_sh):
        bat, d_model = x.shape
        layers, _, seq_len, kv_dim = cache.shape
        n_exp, ff = w1_exp.shape[1], w1_exp.shape[3]
        top_k = expert_ids.shape[2]
        heads = w_q.shape[2] // kv_dim
        assert max(1, (2 * bat * top_k) // (n_exp * group)) == 1 and layers == 2 and chips == 8
        swap = lambda a: jnp.swapaxes(a, -1, -2)
        args = (lengths, x, swap(cache), w_q, swap(w_o), swap(expert_ids), swap(slots), swap(route_w),
                w1_exp, w3_exp, swap(w2_exp), swap(w1_sh), swap(w3_sh), w2_sh)
        vm = lambda a: pltpu.VMEM(a.shape, a.dtype)
        dma = pltpu.SemaphoreType.DMA
        phs = 2 * layers
        hb = bat // 2
        toks = group * hb
        slots_n = n_exp * group
        scratch = [pltpu.SMEM(lengths.shape, lengths.dtype)] + [vm(a) for a in args[1:]] + [
            pltpu.VMEM((group, top_k, toks), F32),
            pltpu.VMEM((layers, 2, slots_n, toks), BF16),
            pltpu.VMEM((layers, 2, 2, 3 * toks // 2, slots_n), BF16),
            pltpu.VMEM((phs, group, hb, d_model), BF16),
            pltpu.VMEM((phs, chips, hb, d_model), F32),
            pltpu.VMEM((phs, chips, hb, d_model), F32),
            pltpu.VMEM((phs, chips, hb, d_model), F32),
            pltpu.VMEM((phs, chips, hb, d_model), F32),
            pltpu.VMEM((phs, chips, hb, d_model), F32),
            pltpu.VMEM((2, hb, d_model), F32),
            pltpu.VMEM((heads * LATENT, d_model), BF16),
            pltpu.VMEM((n_exp * ff, d_model), BF16),
            pltpu.VMEM((2, -(-kv_dim // 128), heads * hb, 128), F32),
            pltpu.VMEM((heads * hb, seq_len), F32),
            pltpu.VMEM((LATENT // 128, heads * hb, 128), F32),
            pltpu.VMEM((slots_n, d_model), BF16),
            pltpu.VMEM((slots_n, d_model), BF16),
            pltpu.VMEM((toks, d_model), F32),
            dma((18,)), dma((layers, bat // 4)),
            dma((phs + 1, chips)), dma((phs + 1, chips + 1)),
            dma((phs,)), dma((phs,)), dma((phs, chips)), dma((phs, chips)), dma((layers, 3)),
        ]
        return pl.pallas_call(
            functools.partial(step_kernel, chips),
            out_shape=jax.ShapeDtypeStruct(x.shape, x.dtype),
            in_specs=[pl.BlockSpec(memory_space=pltpu.HBM)] * len(args),
            out_specs=pl.BlockSpec(memory_space=pltpu.VMEM),
            scratch_shapes=scratch,
            compiler_params=pltpu.CompilerParams(collective_id=0, has_side_effects=True, vmem_limit_bytes=56000000),
        )(*[pltpu.with_memory_space_constraint(a, pltpu.HBM) for a in args])

    return jax.shard_map(device_step, mesh=mesh, in_specs=in_specs, out_specs=P(tok_axes, None), check_vma=False)
```

```python
import functools

import jax
import jax.numpy as jnp
from jax import lax
from jax.experimental import pallas as pl
from jax.experimental.pallas import tpu as pltpu
from jax.sharding import PartitionSpec as P

NORM_EPS = 1e-6
ATT_SCALE = 1.0 / (192.0 ** 0.5)
LATENT = 512
MESH = pl.DeviceIdType.MESH
F32 = jnp.float32
BF16 = jnp.bfloat16


def rms_norm(vals32):
    return vals32 * lax.rsqrt(jnp.mean(vals32 * vals32, axis=-1, keepdims=True) + NORM_EPS)


def dot(lhs, rhs):
    return jnp.dot(lhs, rhs, preferred_element_type=F32)


def dot_t(lhs, rhs):
    return lax.dot_general(lhs, rhs, (((1,), (1,)), ((), ())), preferred_element_type=F32)


def step_kernel(chips, len_hbm, x_hbm, cache_hbm, wq_hbm, wo_hbm, ids_hbm, slots_hbm, rw_hbm, w1_hbm, w3_hbm, w2_hbm,
                w1s_hbm, w3s_hbm, w2s_hbm, out_ref,
                len_ref, x_v, cache_v, wq_v, wo_v, ids_v, slots_v, rw_v, w1_v, w3_v, w2_v, w1s_v, w3s_v, w2s_v,
                rp_all, oh_v, owt_v, g_all, p_buf, own_buf, r1_buf, s_buf, r2_buf, t_buf, a_buf,
                xr_v, wot_v, w2t_v, q_v, sc_v, o_v, xg_v, u_v, sh_v,
                loc_sem, cache_sem, ag_send, ag_recv, rs1_send, rs1_recv, rs2_send, rs2_recv, wq_sem):
    layers, bat, kv_dim, seq_len = cache_v.shape
    d_model = x_v.shape[1]
    heads = wq_v.shape[2] // kv_dim
    n_exp = w1_v.shape[1]
    ff = w1_v.shape[3]
    top_k = ids_v.shape[1]
    group = 2 * chips
    hb = bat // 2
    rows = heads * hb
    toks = group * hb
    half = chips * hb
    quad = 4

    me = lax.axis_index('dp')
    chip = me // 2
    core = me % 2
    other = 1 - core
    q_me = core * chips + chip
    partner = me + 1 - 2 * core

    far_first = (4, 3, 5, 2, 6, 1, 7)
    near_first = (1, 7, 2, 6, 3, 5, 4)

    def chip_at(delta):
        return lax.rem(chip + delta, chips)

    def load(src, dst, idx):
        return pltpu.make_async_copy(src, dst, loc_sem.at[idx])

    small = [load(x_hbm, x_v, 0), load(ids_hbm, ids_v, 1), load(slots_hbm, slots_v, 2), load(rw_hbm, rw_v, 3),
             load(w1s_hbm, w1s_v, 4), load(w3s_hbm, w3s_v, 5), load(w2s_hbm, w2s_v, 6)]
    q_cols = wq_v.shape[2]
    q_part = q_cols // 3
    wq_cp = [[pltpu.make_async_copy(wq_hbm.at[l, :, pl.ds(q_part * c, q_part)], wq_v.at[l, :, pl.ds(q_part * c, q_part)],
                                    wq_sem.at[l, c]) for c in range(3)] for l in range(layers)]
    wo_cp = [load(wo_hbm.at[l], wo_v.at[l], 9 + l) for l in range(layers)]
    w3_cp = [load(w3_hbm.at[l], w3_v.at[l], 11 + l) for l in range(layers)]
    w1_cp = [load(w1_hbm.at[l], w1_v.at[l], 13 + l) for l in range(layers)]
    w2_cp = [load(w2_hbm.at[l], w2_v.at[l], 15 + l) for l in range(layers)]
    cache_cp = [[pltpu.make_async_copy(cache_hbm.at[l, pl.ds(quad * c, quad)], cache_v.at[l, pl.ds(quad * c, quad)],
                                       cache_sem.at[l, c]) for c in range(bat // quad)] for l in range(layers)]

    small[0].start()
    for cp in wq_cp[0]:
        cp.start()
    len_cp = pltpu.make_async_copy(len_hbm, len_ref, loc_sem.at[17])
    for cp in small[1:4]:
        cp.start()
    len_cp.start()
    for cp in cache_cp[0][:2]:
        cp.start()
    wo_cp[0].start()
    for cp in cache_cp[0][2:]:
        cp.start()
    for cp in small[4:]:
        cp.start()

    barrier = pltpu.get_barrier_semaphore()
    for delta in far_first:
        pl.semaphore_signal(barrier, inc=1, device_id={'dp': 2 * chip_at(delta) + core}, device_id_type=MESH)
    pl.semaphore_signal(barrier, inc=1, device_id={'dp': partner}, device_id_type=MESH)

    def remote(src, dst, send, recv, dev):
        return pltpu.make_async_remote_copy(src_ref=src, dst_ref=dst, send_sem=send, recv_sem=recv,
                                            device_id={'dp': dev}, device_id_type=MESH)

    def ag_start(buf, ph):
        mine = buf.at[q_me]
        cps = [remote(mine, mine, ag_send.at[ph, i], ag_recv.at[ph, chip], 2 * chip_at(delta) + core)
               for i, delta in enumerate(far_first)]
        for cp in cps:
            cp.start()
        return cps

    def ag_finish(buf, ph):
        for i, delta in enumerate(near_first):
            src = chip_at(chips - delta)
            q = core * chips + src
            remote(buf.at[q], buf.at[q], ag_send.at[ph, 0], ag_recv.at[ph, src], partner).wait_recv()
        mine = buf.at[pl.ds(core * chips, chips)]
        theirs = buf.at[pl.ds(other * chips, chips)]
        cp = remote(mine, mine, ag_send.at[ph, chips - 1], ag_recv.at[ph, chips], partner)
        cp.start()
        remote(theirs, theirs, ag_send.at[ph, chips - 1], ag_recv.at[ph, chips], partner).wait_recv()
        return [cp]

    for cp in small[1:4]:
        cp.wait()
    pieces = [jnp.where(slots_v[l] >= 0, ids_v[l] + 1, 0).astype(F32) for l in range(layers)]
    pieces += [rw_v[l] for l in range(layers)]
    pieces.append(jnp.zeros((top_k, toks - 2 * layers * bat), F32))
    rp_all[q_me] = jnp.concatenate(pieces, axis=1)

    pl.semaphore_wait(barrier, chips)
    sends = ag_start(rp_all, 2 * layers)

    small[0].wait()
    xr_v[...] = x_v[...].astype(F32).reshape(2, hb, d_model)

    def transpose_wo(l):
        wo_cp[l].wait()
        for k in range(heads * LATENT // 128):
            wot_v[128 * k:128 * (k + 1), :] = wo_v[l, :, 128 * k:128 * (k + 1)].T

    def transpose_w2(l):
        w2_cp[l].wait()
        for n in range(n_exp):
            w2t_v[ff * n:ff * (n + 1), :] = w2_v[l, n].T

    def transpose_cache(c):
        cache_cp[1][c].wait()
        for b in range(quad * c, quad * (c + 1)):
            cache_v[0, b, 0:LATENT, :] = cache_v[1, b, 0:LATENT, :].T

    def attention(l, hf):
        halves = (0, 1) if l == 0 else (hf,)
        if l > 0 or hf == 0:
            x_in = xr_v[...].reshape(bat, d_model) if l == 0 else xr_v[hf]
            hidden = rms_norm(x_in).astype(BF16)
            q = []
            if l > 0 and hf == 0:
                for cp in wq_cp[l]:
                    cp.wait()
            for c in range(3):
                if l == 0:
                    wq_cp[l][c].wait()
                q.append(dot(hidden, wq_v[l, :, q_part * c:q_part * (c + 1)]))
            q = jnp.concatenate(q, axis=1)
            for hd in range(heads):
                part = q if hd == 0 else pltpu.roll(q, q_cols - hd * kv_dim, 1)
                for i, h in enumerate(halves):
                    for k in range(q_v.shape[1]):
                        q_v[h, k, pl.ds(hd, hb, stride=heads), :] = part[hb * i:hb * (i + 1), 128 * k:128 * (k + 1)]
        if l == 0 and hf == 0:
            len_cp.wait()
        for grp in (((0,), (1,)) if l == 0 and hf == 0 else ((0, 1),)):
            first, count = heads * quad * grp[0], heads * quad * len(grp)
            seqs = range(quad * grp[0], quad * (grp[-1] + 1))
            if l == 0:
                for c in grp:
                    cache_cp[l][2 * hf + c].wait()
            for b in seqs:
                qb = jnp.concatenate([q_v[hf, k, heads * b:heads * (b + 1), :] for k in range(q_v.shape[1])], axis=1)
                qb = qb[:, :kv_dim].astype(BF16)
                sc_v[heads * b:heads * (b + 1), :] = dot(qb, cache_v[l, hf * hb + b])
            row_tok = (lax.broadcasted_iota(jnp.int32, (count, 1), 0) + first) // heads
            lens = jnp.zeros((count, 1), jnp.int32)
            for b in seqs:
                lens = jnp.where(row_tok == b, len_ref[hf * hb + b], lens)
            valid = lax.broadcasted_iota(jnp.int32, (count, seq_len), 1) < lens
            scores = jnp.where(valid, sc_v[first:first + count, :] * ATT_SCALE, -jnp.inf)
            top = jnp.max(scores, axis=1, keepdims=True)
            ex = jnp.exp(scores - top)
            sc_v[first:first + count, :] = ex / jnp.sum(ex, axis=1, keepdims=True)
            for b in seqs:
                pb = sc_v[heads * b:heads * (b + 1), :].astype(BF16)
                if l == 0:
                    ob = dot_t(pb, cache_v[0, hf * hb + b, 0:LATENT, :])
                else:
                    ob = dot(pb, cache_v[0, hf * hb + b, 0:LATENT, :])
                for k in range(o_v.shape[0]):
                    o_v[k, heads * b:heads * (b + 1), :] = ob[:, 128 * k:128 * (k + 1)]
            if l == 0 and hf == 0 and grp[0] == 0:
                for cps in (w2_cp, w3_cp, w1_cp):
                    cps[0].start()
        attn = jnp.concatenate([o_v[k, pl.ds(hd, hb, stride=heads), :] for hd in range(heads)
                                for k in range(o_v.shape[0])], axis=1).astype(BF16)
        if l == 0:
            if hf == 0:
                wo_cp[0].wait()
            proj = jnp.concatenate([dot_t(attn, wo_v[0, 0:256]), dot_t(attn, wo_v[0, 256:d_model])], axis=1)
        else:
            proj = jnp.concatenate([dot(attn, wot_v[:, 0:256]), dot(attn, wot_v[:, 256:d_model])], axis=1)
        resid = (xr_v[hf] + proj).astype(BF16).astype(F32)
        xr_v[hf] = resid
        g_all[2 * l + hf, q_me] = rms_norm(resid).astype(BF16)

    def gather_field(e):
        lane_q = lax.broadcasted_iota(jnp.int32, (top_k, toks), 1) // hb
        field = jnp.zeros((top_k, toks), F32)
        for q in range(group):
            shift = (q - e) * hb % toks
            tile = rp_all[q]
            field = jnp.where(lane_q == q, tile if shift == 0 else pltpu.roll(tile, shift, 1), field)
        return field

    def build_masks(l):
        base = me * n_exp + 1
        want = (lax.broadcasted_iota(jnp.int32, (n_exp, toks), 0) + base).astype(F32)
        lane_src = lax.broadcasted_iota(jnp.int32, (group, toks), 1) // hb
        own_src = lane_src == lax.broadcasted_iota(jnp.int32, (group, toks), 0)
        for hf in range(2):
            code = gather_field(2 * l + hf)
            wval = gather_field(2 * (layers + l) + hf)
            member = jnp.zeros((n_exp, toks), F32)
            weight = jnp.zeros((n_exp, toks), F32)
            for j in range(top_k):
                hit = code[j:j + 1, :] == want
                member = jnp.where(hit, 1.0, member)
                weight = jnp.where(hit, wval[j:j + 1, :], weight)
            onehot = [jnp.where(own_src, member[n:n + 1, :], 0.0) for n in range(n_exp)]
            oh_v[l, hf] = jnp.concatenate(onehot, axis=0).astype(BF16)
            ow = jnp.concatenate([jnp.where(own_src, weight[n:n + 1, :], 0.0) for n in range(n_exp)], axis=0)
            owt = ow.T
            hi = owt.astype(BF16)
            rest = owt - hi.astype(F32)
            mid = rest.astype(BF16)
            low = (rest - mid.astype(F32)).astype(BF16)
            for k in range(2):
                for i, term in enumerate((hi, mid, low)):
                    owt_v[l, hf, k, i * half:(i + 1) * half, :] = term[k * half:(k + 1) * half, :]

    def experts(l, hf, between=None):
        ph = 2 * l + hf
        g_in = g_all[ph].reshape(toks, d_model)
        xg_v[...] = dot(oh_v[l, hf], g_in).astype(BF16)
        if hf == 0:
            for cps in (w3_cp, w1_cp):
                cps[l].wait()

        def first_layer(pair):
            hid = []
            for e in range(2):
                n = 2 * pair + e
                xin = xg_v[group * n:group * (n + 1), :]
                w31 = jnp.concatenate([w3_v[l, n], w1_v[l, n]], axis=1)
                both = dot(xin, w31)
                hid.append((jax.nn.silu(both[:, :ff]) * both[:, ff:]).astype(BF16))
            zero = jnp.zeros((group, ff), BF16)
            return jnp.concatenate([jnp.concatenate([hid[0], zero], axis=1),
                                    jnp.concatenate([zero, hid[1]], axis=1)], axis=0)

        def second_layer(pair, lhs):
            u_v[2 * group * pair:2 * group * (pair + 1), :] = dot(lhs, w2t_v[2 * ff * pair:2 * ff * (pair + 1), :]).astype(BF16)

        def shared_expert():
            gate = dot_t(g_in, w3s_v[l])
            up = dot_t(g_in, w1s_v[l])
            shared_h = (jax.nn.silu(gate) * up).astype(BF16)
            sh_v[...] = dot(shared_h, w2s_v[l])

        pairs = n_exp // 2
        ready = first_layer(0)
        for pair in range(pairs):
            coming = first_layer(pair + 1) if pair < pairs - 1 else None
            second_layer(pair, ready)
            ready = coming
            if pair == 2:
                shared_expert()
            if pair == 2 and between is not None:
                between()

        def part(k):
            sel = pl.ds(pl.multiple_of(k * half, half), half)
            three = dot(owt_v[l, hf, k], u_v[...])
            return sh_v[sel, :] + (three[:half] + three[half:2 * half] + three[2 * half:])

        p_buf[ph] = part(other).reshape(chips, hb, d_model)
        first = remote(p_buf.at[ph], r1_buf.at[ph], rs1_send.at[ph], rs1_recv.at[ph], partner)
        first.start()
        own_buf[ph] = part(core).reshape(chips, hb, d_model)
        return first

    def second_stage(l, hf, first):
        ph = 2 * l + hf
        first.wait_recv()
        s_buf[ph] = own_buf[ph] + r1_buf[ph]
        cps = [first]
        hops = ((4, 2, t_buf.at[ph, 0], 4), (3, 1, t_buf.at[ph, 1], 5), (chips - 3, chips - 1, t_buf.at[ph, 2], 6),
                (1, 1, r2_buf.at[ph, 0], 0), (chips - 1, chips - 1, r2_buf.at[ph, 1], 1))
        for i, (owner, to, dst, sem) in enumerate(hops):
            cps.append(remote(s_buf.at[ph, chip_at(owner)], dst, rs2_send.at[ph, i], rs2_recv.at[ph, sem],
                              2 * chip_at(to) + core))
            cps[-1].start()
        return cps

    def arrived(dst, ph, sem):
        remote(dst, dst, rs2_send.at[ph, 0], rs2_recv.at[ph, sem], partner).wait_recv()

    def third_stage(l, hf):
        ph = 2 * l + hf
        for i in range(3):
            arrived(t_buf.at[ph, i], ph, 4 + i)
        ahead, behind = chip_at(2), chip_at(chips - 2)
        a_buf[ph, 0] = s_buf[ph, ahead] + (t_buf[ph, 0] + t_buf[ph, 1])
        cps = [remote(a_buf.at[ph, 0], r2_buf.at[ph, 2], rs2_send.at[ph, 5], rs2_recv.at[ph, 2], 2 * ahead + core)]
        cps[0].start()
        a_buf[ph, 1] = s_buf[ph, behind] + t_buf[ph, 2]
        cps.append(remote(a_buf.at[ph, 1], r2_buf.at[ph, 3], rs2_send.at[ph, 6], rs2_recv.at[ph, 3], 2 * behind + core))
        cps[1].start()
        return cps

    def finish(l, hf):
        ph = 2 * l + hf
        tot = s_buf[ph, chip]
        for i in range(4):
            arrived(r2_buf.at[ph, i], ph, i)
            tot = tot + r2_buf[ph, i]
        xr_v[hf] = (xr_v[hf] + tot).astype(BF16).astype(F32)

    attention(0, 0)
    sends += ag_start(g_all.at[0], 0)
    attention(0, 1)
    sends += ag_start(g_all.at[1], 1)
    for cp in cache_cp[1]:
        cp.start()
    for cp in small[4:]:
        cp.wait()
    sends += ag_finish(rp_all, 2 * layers)
    build_masks(0)
    transpose_w2(0)
    sends += ag_finish(g_all.at[0], 0)
    for cp in wq_cp[1] + [wo_cp[1]]:
        cp.start()
    later = []
    first_a = experts(0, 0)
    sends += ag_finish(g_all.at[1], 1)
    for cp_list in (w3_cp, w1_cp, w2_cp):
        cp_list[1].start()
    first_b = experts(0, 1, lambda: later.extend(second_stage(0, 0, first_a)))
    build_masks(1)
    transpose_cache(0)
    later += second_stage(0, 1, first_b)
    later += third_stage(0, 0)
    for c in range(1, bat // quad):
        transpose_cache(c)
    transpose_wo(1)
    later += third_stage(0, 1)
    finish(0, 0)
    attention(1, 0)
    sends += ag_start(g_all.at[2], 2)
    finish(0, 1)
    attention(1, 1)
    sends += ag_start(g_all.at[3], 3)
    transpose_w2(1)
    sends += ag_finish(g_all.at[2], 2)
    first_a = experts(1, 0)
    sends += ag_finish(g_all.at[3], 3)
    first_b = experts(1, 1, lambda: later.extend(second_stage(1, 0, first_a)))
    sends += later + third_stage(1, 0) + second_stage(1, 1, first_b)
    sends += third_stage(1, 1)
    for hf in range(2):
        finish(layers - 1, hf)
    for cp in sends:
        cp.wait_send()
    out_ref[...] = xr_v[...].reshape(bat, d_model).astype(BF16)


def solution(mesh):
    group = mesh.shape['dp']
    chips = group // 2
    tok_axes = ('replica', 'dp')
    in_specs = (
        P(tok_axes, None), P(tok_axes), P(None, tok_axes, None, None),
        P(None, None, None), P(None, None, None),
        P(None, tok_axes, None), P(None, tok_axes, None), P(None, tok_axes, None),
        P(None, 'dp', None, None), P(None, 'dp', None, None), P(None, 'dp', None, None),
        P(None, None, 'dp'), P(None, None, 'dp'), P(None, 'dp', None),
    )

    def device_step(x, lengths, cache, w_q, w_o, expert_ids, slots, route_w, w1_exp, w3_exp, w2_exp, w1_sh, w3_sh, w2_sh):
        bat, d_model = x.shape
        layers, _, seq_len, kv_dim = cache.shape
        n_exp, ff = w1_exp.shape[1], w1_exp.shape[3]
        top_k = expert_ids.shape[2]
        heads = w_q.shape[2] // kv_dim
        assert max(1, (2 * bat * top_k) // (n_exp * group)) == 1 and layers == 2 and chips == 8
        swap = lambda a: jnp.swapaxes(a, -1, -2)
        args = (lengths, x, swap(cache), w_q, swap(w_o), swap(expert_ids), swap(slots), swap(route_w),
                w1_exp, w3_exp, swap(w2_exp), swap(w1_sh), swap(w3_sh), w2_sh)
        vm = lambda a: pltpu.VMEM(a.shape, a.dtype)
        dma = pltpu.SemaphoreType.DMA
        phs = 2 * layers
        hb = bat // 2
        toks = group * hb
        slots_n = n_exp * group
        scratch = [pltpu.SMEM(lengths.shape, lengths.dtype)] + [vm(a) for a in args[1:]] + [
            pltpu.VMEM((group, top_k, toks), F32),
            pltpu.VMEM((layers, 2, slots_n, toks), BF16),
            pltpu.VMEM((layers, 2, 2, 3 * toks // 2, slots_n), BF16),
            pltpu.VMEM((phs, group, hb, d_model), BF16),
            pltpu.VMEM((phs, chips, hb, d_model), F32),
            pltpu.VMEM((phs, chips, hb, d_model), F32),
            pltpu.VMEM((phs, chips, hb, d_model), F32),
            pltpu.VMEM((phs, chips, hb, d_model), F32),
            pltpu.VMEM((phs, 4, hb, d_model), F32),
            pltpu.VMEM((phs, 3, hb, d_model), F32),
            pltpu.VMEM((phs, 2, hb, d_model), F32),
            pltpu.VMEM((2, hb, d_model), F32),
            pltpu.VMEM((heads * LATENT, d_model), BF16),
            pltpu.VMEM((n_exp * ff, d_model), BF16),
            pltpu.VMEM((2, -(-kv_dim // 128), heads * hb, 128), F32),
            pltpu.VMEM((heads * hb, seq_len), F32),
            pltpu.VMEM((LATENT // 128, heads * hb, 128), F32),
            pltpu.VMEM((slots_n, d_model), BF16),
            pltpu.VMEM((slots_n, d_model), BF16),
            pltpu.VMEM((toks, d_model), F32),
            dma((18,)), dma((layers, bat // 4)),
            dma((phs + 1, chips)), dma((phs + 1, chips + 1)),
            dma((phs,)), dma((phs,)), dma((phs, chips)), dma((phs, chips)), dma((layers, 3)),
        ]
        return pl.pallas_call(
            functools.partial(step_kernel, chips),
            out_shape=jax.ShapeDtypeStruct(x.shape, x.dtype),
            in_specs=[pl.BlockSpec(memory_space=pltpu.HBM)] * len(args),
            out_specs=pl.BlockSpec(memory_space=pltpu.VMEM),
            scratch_shapes=scratch,
            compiler_params=pltpu.CompilerParams(collective_id=0, has_side_effects=True, vmem_limit_bytes=56000000),
        )(*[pltpu.with_memory_space_constraint(a, pltpu.HBM) for a in args])

    return jax.shard_map(device_step, mesh=mesh, in_specs=in_specs, out_specs=P(tok_axes, None), check_vma=False)
```

```python
import functools

import jax
import jax.numpy as jnp
from jax import lax
from jax.experimental import pallas as pl
from jax.experimental.pallas import tpu as pltpu
from jax.sharding import PartitionSpec as P

NORM_EPS = 1e-6
ATT_SCALE = 1.0 / (192.0 ** 0.5)
LATENT = 512
MESH = pl.DeviceIdType.MESH
F32 = jnp.float32
BF16 = jnp.bfloat16


def rms_norm(vals32):
    return vals32 * lax.rsqrt(jnp.mean(vals32 * vals32, axis=-1, keepdims=True) + NORM_EPS)


def dot(lhs, rhs):
    return jnp.dot(lhs, rhs, preferred_element_type=F32)


def dot_t(lhs, rhs):
    return lax.dot_general(lhs, rhs, (((1,), (1,)), ((), ())), preferred_element_type=F32)


def step_kernel(chips, len_hbm, x_hbm, cache_hbm, wq_hbm, wo_hbm, ids_hbm, slots_hbm, rw_hbm, w1_hbm, w3_hbm, w2_hbm,
                w1s_hbm, w3s_hbm, w2s_hbm, out_ref,
                len_ref, x_v, cache_v, wq_v, wo_v, ids_v, slots_v, rw_v, w1_v, w3_v, w2_v, w1s_v, w3s_v, w2s_v,
                rp_all, oh_v, owt_v, g_all, p_buf, own_buf, r1_buf, s_buf, r2_buf,
                xr_v, wot_v, w2t_v, q_v, sc_v, o_v, xg_v, u_v, sh_v,
                loc_sem, cache_sem, ag_send, ag_recv, rs1_send, rs1_recv, rs2_send, rs2_recv, wq_sem):
    layers, bat, kv_dim, seq_len = cache_v.shape
    d_model = x_v.shape[1]
    heads = wq_v.shape[2] // kv_dim
    n_exp = w1_v.shape[1]
    ff = w1_v.shape[3]
    top_k = ids_v.shape[1]
    group = 2 * chips
    hb = bat // 2
    rows = heads * hb
    toks = group * hb
    half = chips * hb
    quad = 4

    me = lax.axis_index('dp')
    chip = me // 2
    core = me % 2
    other = 1 - core
    q_me = core * chips + chip
    partner = me + 1 - 2 * core

    far_first = (4, 3, 5, 2, 6, 1, 7)
    near_first = (1, 7, 2, 6, 3, 5, 4)

    def chip_at(delta):
        return lax.rem(chip + delta, chips)

    def load(src, dst, idx):
        return pltpu.make_async_copy(src, dst, loc_sem.at[idx])

    small = [load(x_hbm, x_v, 0), load(ids_hbm, ids_v, 1), load(slots_hbm, slots_v, 2), load(rw_hbm, rw_v, 3),
             load(w1s_hbm, w1s_v, 4), load(w3s_hbm, w3s_v, 5), load(w2s_hbm, w2s_v, 6)]
    q_cols = wq_v.shape[2]
    q_part = q_cols // 3
    wq_cp = [[pltpu.make_async_copy(wq_hbm.at[l, :, pl.ds(q_part * c, q_part)], wq_v.at[l, :, pl.ds(q_part * c, q_part)],
                                    wq_sem.at[l, c]) for c in range(3)] for l in range(layers)]
    wo_cp = [load(wo_hbm.at[l], wo_v.at[l], 9 + l) for l in range(layers)]
    w3_cp = [load(w3_hbm.at[l], w3_v.at[l], 11 + l) for l in range(layers)]
    w1_cp = [load(w1_hbm.at[l], w1_v.at[l], 13 + l) for l in range(layers)]
    w2_cp = [load(w2_hbm.at[l], w2_v.at[l], 15 + l) for l in range(layers)]
    cache_cp = [[pltpu.make_async_copy(cache_hbm.at[l, pl.ds(quad * c, quad)], cache_v.at[l, pl.ds(quad * c, quad)],
                                       cache_sem.at[l, c]) for c in range(bat // quad)] for l in range(layers)]

    small[0].start()
    for cp in wq_cp[0]:
        cp.start()
    len_cp = pltpu.make_async_copy(len_hbm, len_ref, loc_sem.at[17])
    for cp in small[1:4]:
        cp.start()
    len_cp.start()
    for cp in cache_cp[0][:2]:
        cp.start()
    wo_cp[0].start()
    for cp in cache_cp[0][2:]:
        cp.start()
    for cp in small[4:]:
        cp.start()

    barrier = pltpu.get_barrier_semaphore()
    for delta in far_first:
        pl.semaphore_signal(barrier, inc=1, device_id={'dp': 2 * chip_at(delta) + core}, device_id_type=MESH)
    pl.semaphore_signal(barrier, inc=1, device_id={'dp': partner}, device_id_type=MESH)

    def remote(src, dst, send, recv, dev):
        return pltpu.make_async_remote_copy(src_ref=src, dst_ref=dst, send_sem=send, recv_sem=recv,
                                            device_id={'dp': dev}, device_id_type=MESH)

    def ag_start(buf, ph):
        mine = buf.at[q_me]
        cps = [remote(mine, mine, ag_send.at[ph, i], ag_recv.at[ph, chip], 2 * chip_at(delta) + core)
               for i, delta in enumerate(far_first)]
        for cp in cps:
            cp.start()
        return cps

    def ag_forward(buf, ph):
        for i, delta in enumerate(near_first):
            src = chip_at(chips - delta)
            q = core * chips + src
            remote(buf.at[q], buf.at[q], ag_send.at[ph, 0], ag_recv.at[ph, src], partner).wait_recv()
        mine = buf.at[pl.ds(core * chips, chips)]
        cp = remote(mine, mine, ag_send.at[ph, chips - 1], ag_recv.at[ph, chips], partner)
        cp.start()
        return [cp]

    def ag_wait(buf, ph):
        theirs = buf.at[pl.ds(other * chips, chips)]
        remote(theirs, theirs, ag_send.at[ph, chips - 1], ag_recv.at[ph, chips], partner).wait_recv()

    def ag_finish(buf, ph):
        cps = ag_forward(buf, ph)
        ag_wait(buf, ph)
        return cps

    for cp in small[1:4]:
        cp.wait()
    pieces = [jnp.where(slots_v[l] >= 0, ids_v[l] + 1, 0).astype(F32) for l in range(layers)]
    pieces += [rw_v[l] for l in range(layers)]
    pieces.append(jnp.zeros((top_k, toks - 2 * layers * bat), F32))
    rp_all[q_me] = jnp.concatenate(pieces, axis=1)

    pl.semaphore_wait(barrier, chips)
    sends = ag_start(rp_all, 2 * layers)

    small[0].wait()
    xr_v[...] = x_v[...].astype(F32).reshape(2, hb, d_model)

    def transpose_wo(l):
        wo_cp[l].wait()
        for k in range(heads * LATENT // 128):
            wot_v[128 * k:128 * (k + 1), :] = wo_v[l, :, 128 * k:128 * (k + 1)].T

    def transpose_w2(l):
        w2_cp[l].wait()
        for n in range(n_exp):
            w2t_v[ff * n:ff * (n + 1), :] = w2_v[l, n].T

    def transpose_cache(c):
        cache_cp[1][c].wait()
        for b in range(quad * c, quad * (c + 1)):
            cache_v[0, b, 0:LATENT, :] = cache_v[1, b, 0:LATENT, :].T

    def attention(l, hf):
        halves = (0, 1) if l == 0 else (hf,)
        if l > 0 or hf == 0:
            x_in = xr_v[...].reshape(bat, d_model) if l == 0 else xr_v[hf]
            hidden = rms_norm(x_in).astype(BF16)
            q = []
            if l > 0 and hf == 0:
                for cp in wq_cp[l]:
                    cp.wait()
            for c in range(3):
                if l == 0:
                    wq_cp[l][c].wait()
                q.append(dot(hidden, wq_v[l, :, q_part * c:q_part * (c + 1)]))
            q = jnp.concatenate(q, axis=1)
            for hd in range(heads):
                part = q if hd == 0 else pltpu.roll(q, q_cols - hd * kv_dim, 1)
                for i, h in enumerate(halves):
                    for k in range(q_v.shape[1]):
                        q_v[h, k, pl.ds(hd, hb, stride=heads), :] = part[hb * i:hb * (i + 1), 128 * k:128 * (k + 1)]
        if l == 0 and hf == 0:
            len_cp.wait()
        for grp in (((0,), (1,)) if l == 0 and hf == 0 else ((0, 1),)):
            first, count = heads * quad * grp[0], heads * quad * len(grp)
            seqs = range(quad * grp[0], quad * (grp[-1] + 1))
            if l == 0:
                for c in grp:
                    cache_cp[l][2 * hf + c].wait()
            for b in seqs:
                qb = jnp.concatenate([q_v[hf, k, heads * b:heads * (b + 1), :] for k in range(q_v.shape[1])], axis=1)
                qb = qb[:, :kv_dim].astype(BF16)
                sc_v[heads * b:heads * (b + 1), :] = dot(qb, cache_v[l, hf * hb + b])
            row_tok = (lax.broadcasted_iota(jnp.int32, (count, 1), 0) + first) // heads
            lens = jnp.zeros((count, 1), jnp.int32)
            for b in seqs:
                lens = jnp.where(row_tok == b, len_ref[hf * hb + b], lens)
            valid = lax.broadcasted_iota(jnp.int32, (count, seq_len), 1) < lens
            scores = jnp.where(valid, sc_v[first:first + count, :] * ATT_SCALE, -jnp.inf)
            top = jnp.max(scores, axis=1, keepdims=True)
            ex = jnp.exp(scores - top)
            sc_v[first:first + count, :] = ex / jnp.sum(ex, axis=1, keepdims=True)
            for b in seqs:
                pb = sc_v[heads * b:heads * (b + 1), :].astype(BF16)
                if l == 0:
                    ob = dot_t(pb, cache_v[0, hf * hb + b, 0:LATENT, :])
                else:
                    ob = dot(pb, cache_v[0, hf * hb + b, 0:LATENT, :])
                for k in range(o_v.shape[0]):
                    o_v[k, heads * b:heads * (b + 1), :] = ob[:, 128 * k:128 * (k + 1)]
            if l == 0 and hf == 0 and grp[0] == 0:
                for cps in (w2_cp, w3_cp, w1_cp):
                    cps[0].start()
        attn = jnp.concatenate([o_v[k, pl.ds(hd, hb, stride=heads), :] for hd in range(heads)
                                for k in range(o_v.shape[0])], axis=1).astype(BF16)
        if l == 0:
            if hf == 0:
                wo_cp[0].wait()
            proj = jnp.concatenate([dot_t(attn, wo_v[0, 0:256]), dot_t(attn, wo_v[0, 256:d_model])], axis=1)
        else:
            proj = jnp.concatenate([dot(attn, wot_v[:, 0:256]), dot(attn, wot_v[:, 256:d_model])], axis=1)
        resid = (xr_v[hf] + proj).astype(BF16).astype(F32)
        xr_v[hf] = resid
        g_all[2 * l + hf, q_me] = rms_norm(resid).astype(BF16)

    def gather_field(e):
        lane_q = lax.broadcasted_iota(jnp.int32, (top_k, toks), 1) // hb
        field = jnp.zeros((top_k, toks), F32)
        for q in range(group):
            shift = (q - e) * hb % toks
            tile = rp_all[q]
            field = jnp.where(lane_q == q, tile if shift == 0 else pltpu.roll(tile, shift, 1), field)
        return field

    def build_masks(l):
        base = me * n_exp + 1
        want = (lax.broadcasted_iota(jnp.int32, (n_exp, toks), 0) + base).astype(F32)
        lane_src = lax.broadcasted_iota(jnp.int32, (group, toks), 1) // hb
        own_src = lane_src == lax.broadcasted_iota(jnp.int32, (group, toks), 0)
        for hf in range(2):
            code = gather_field(2 * l + hf)
            wval = gather_field(2 * (layers + l) + hf)
            member = jnp.zeros((n_exp, toks), F32)
            weight = jnp.zeros((n_exp, toks), F32)
            for j in range(top_k):
                hit = code[j:j + 1, :] == want
                member = jnp.where(hit, 1.0, member)
                weight = jnp.where(hit, wval[j:j + 1, :], weight)
            onehot = [jnp.where(own_src, member[n:n + 1, :], 0.0) for n in range(n_exp)]
            oh_v[l, hf] = jnp.concatenate(onehot, axis=0).astype(BF16)
            ow = jnp.concatenate([jnp.where(own_src, weight[n:n + 1, :], 0.0) for n in range(n_exp)], axis=0)
            owt = ow.T
            hi = owt.astype(BF16)
            rest = owt - hi.astype(F32)
            mid = rest.astype(BF16)
            low = (rest - mid.astype(F32)).astype(BF16)
            for k in range(2):
                for i, term in enumerate((hi, mid, low)):
                    owt_v[l, hf, k, i * half:(i + 1) * half, :] = term[k * half:(k + 1) * half, :]

    def experts(l, hf, between=None):
        ph = 2 * l + hf
        g_in = g_all[ph].reshape(toks, d_model)
        xg_v[...] = dot(oh_v[l, hf], g_in).astype(BF16)
        if hf == 0:
            for cps in (w3_cp, w1_cp):
                cps[l].wait()

        def first_layer(pair):
            hid = []
            for e in range(2):
                n = 2 * pair + e
                xin = xg_v[group * n:group * (n + 1), :]
                w31 = jnp.concatenate([w3_v[l, n], w1_v[l, n]], axis=1)
                both = dot(xin, w31)
                hid.append((jax.nn.silu(both[:, :ff]) * both[:, ff:]).astype(BF16))
            zero = jnp.zeros((group, ff), BF16)
            return jnp.concatenate([jnp.concatenate([hid[0], zero], axis=1),
                                    jnp.concatenate([zero, hid[1]], axis=1)], axis=0)

        def second_layer(pair, lhs):
            u_v[2 * group * pair:2 * group * (pair + 1), :] = dot(lhs, w2t_v[2 * ff * pair:2 * ff * (pair + 1), :]).astype(BF16)

        def shared_expert():
            gate = dot_t(g_in, w3s_v[l])
            up = dot_t(g_in, w1s_v[l])
            shared_h = (jax.nn.silu(gate) * up).astype(BF16)
            sh_v[...] = dot(shared_h, w2s_v[l])

        pairs = n_exp // 2
        ready = first_layer(0)
        for pair in range(pairs):
            coming = first_layer(pair + 1) if pair < pairs - 1 else None
            second_layer(pair, ready)
            ready = coming
            if pair == 2:
                shared_expert()
            if pair == 2 and between is not None:
                between()

        def part(k):
            sel = pl.ds(pl.multiple_of(k * half, half), half)
            three = dot(owt_v[l, hf, k], u_v[...])
            return sh_v[sel, :] + (three[:half] + three[half:2 * half] + three[2 * half:])

        p_buf[ph] = part(other).reshape(chips, hb, d_model)
        first = remote(p_buf.at[ph], r1_buf.at[ph], rs1_send.at[ph], rs1_recv.at[ph], partner)
        first.start()
        own_buf[ph] = part(core).reshape(chips, hb, d_model)
        return first

    def second_stage(l, hf, first):
        ph = 2 * l + hf
        first.wait_recv()
        s_buf[ph] = own_buf[ph] + r1_buf[ph]
        cps = [first]
        for i, delta in enumerate(far_first):
            dst = chip_at(delta)
            cp = remote(s_buf.at[ph, dst], r2_buf.at[ph, chip], rs2_send.at[ph, i], rs2_recv.at[ph, chip], 2 * dst + core)
            cp.start()
            cps.append(cp)
        r2_buf[ph, chip] = s_buf[ph, chip]
        return cps

    def finish(l, hf):
        ph = 2 * l + hf
        for i, delta in enumerate(near_first):
            src = chip_at(chips - delta)
            remote(s_buf.at[ph, src], r2_buf.at[ph, src], rs2_send.at[ph, 0], rs2_recv.at[ph, src], partner).wait_recv()
        tot = r2_buf[ph, 0]
        for j in range(1, chips):
            tot = tot + r2_buf[ph, j]
        xr_v[hf] = (xr_v[hf] + tot).astype(BF16).astype(F32)

    attention(0, 0)
    sends += ag_start(g_all.at[0], 0)
    attention(0, 1)
    sends += ag_start(g_all.at[1], 1)
    for cp in cache_cp[1]:
        cp.start()
    for cp in small[4:]:
        cp.wait()
    sends += ag_finish(rp_all, 2 * layers)
    build_masks(0)
    sends += ag_forward(g_all.at[0], 0)
    transpose_w2(0)
    ag_wait(g_all.at[0], 0)
    for cp in wq_cp[1] + [wo_cp[1]]:
        cp.start()
    later = []
    first_a = experts(0, 0)
    sends += ag_forward(g_all.at[1], 1)
    for cp_list in (w3_cp, w1_cp, w2_cp):
        cp_list[1].start()
    later += second_stage(0, 0, first_a)
    ag_wait(g_all.at[1], 1)
    first_b = experts(0, 1)
    build_masks(1)
    transpose_cache(0)
    later += second_stage(0, 1, first_b)
    for c in range(1, bat // quad):
        transpose_cache(c)
    transpose_wo(1)
    finish(0, 0)
    attention(1, 0)
    sends += ag_start(g_all.at[2], 2)
    finish(0, 1)
    attention(1, 1)
    sends += ag_start(g_all.at[3], 3)
    transpose_w2(1)
    sends += ag_finish(g_all.at[2], 2)
    first_a = experts(1, 0)
    sends += ag_finish(g_all.at[3], 3)
    first_b = experts(1, 1, lambda: later.extend(second_stage(1, 0, first_a)))
    sends += later + second_stage(1, 1, first_b)
    for hf in range(2):
        finish(layers - 1, hf)
    for cp in sends:
        cp.wait_send()
    out_ref[...] = xr_v[...].reshape(bat, d_model).astype(BF16)


def solution(mesh):
    group = mesh.shape['dp']
    chips = group // 2
    tok_axes = ('replica', 'dp')
    in_specs = (
        P(tok_axes, None), P(tok_axes), P(None, tok_axes, None, None),
        P(None, None, None), P(None, None, None),
        P(None, tok_axes, None), P(None, tok_axes, None), P(None, tok_axes, None),
        P(None, 'dp', None, None), P(None, 'dp', None, None), P(None, 'dp', None, None),
        P(None, None, 'dp'), P(None, None, 'dp'), P(None, 'dp', None),
    )

    def device_step(x, lengths, cache, w_q, w_o, expert_ids, slots, route_w, w1_exp, w3_exp, w2_exp, w1_sh, w3_sh, w2_sh):
        bat, d_model = x.shape
        layers, _, seq_len, kv_dim = cache.shape
        n_exp, ff = w1_exp.shape[1], w1_exp.shape[3]
        top_k = expert_ids.shape[2]
        heads = w_q.shape[2] // kv_dim
        assert max(1, (2 * bat * top_k) // (n_exp * group)) == 1 and layers == 2 and chips == 8
        swap = lambda a: jnp.swapaxes(a, -1, -2)
        args = (lengths, x, swap(cache), w_q, swap(w_o), swap(expert_ids), swap(slots), swap(route_w),
                w1_exp, w3_exp, swap(w2_exp), swap(w1_sh), swap(w3_sh), w2_sh)
        vm = lambda a: pltpu.VMEM(a.shape, a.dtype)
        dma = pltpu.SemaphoreType.DMA
        phs = 2 * layers
        hb = bat // 2
        toks = group * hb
        slots_n = n_exp * group
        scratch = [pltpu.SMEM(lengths.shape, lengths.dtype)] + [vm(a) for a in args[1:]] + [
            pltpu.VMEM((group, top_k, toks), F32),
            pltpu.VMEM((layers, 2, slots_n, toks), BF16),
            pltpu.VMEM((layers, 2, 2, 3 * toks // 2, slots_n), BF16),
            pltpu.VMEM((phs, group, hb, d_model), BF16),
            pltpu.VMEM((phs, chips, hb, d_model), F32),
            pltpu.VMEM((phs, chips, hb, d_model), F32),
            pltpu.VMEM((phs, chips, hb, d_model), F32),
            pltpu.VMEM((phs, chips, hb, d_model), F32),
            pltpu.VMEM((phs, chips, hb, d_model), F32),
            pltpu.VMEM((2, hb, d_model), F32),
            pltpu.VMEM((heads * LATENT, d_model), BF16),
            pltpu.VMEM((n_exp * ff, d_model), BF16),
            pltpu.VMEM((2, -(-kv_dim // 128), heads * hb, 128), F32),
            pltpu.VMEM((heads * hb, seq_len), F32),
            pltpu.VMEM((LATENT // 128, heads * hb, 128), F32),
            pltpu.VMEM((slots_n, d_model), BF16),
            pltpu.VMEM((slots_n, d_model), BF16),
            pltpu.VMEM((toks, d_model), F32),
            dma((18,)), dma((layers, bat // 4)),
            dma((phs + 1, chips)), dma((phs + 1, chips + 1)),
            dma((phs,)), dma((phs,)), dma((phs, chips)), dma((phs, chips)), dma((layers, 3)),
        ]
        return pl.pallas_call(
            functools.partial(step_kernel, chips),
            out_shape=jax.ShapeDtypeStruct(x.shape, x.dtype),
            in_specs=[pl.BlockSpec(memory_space=pltpu.HBM)] * len(args),
            out_specs=pl.BlockSpec(memory_space=pltpu.VMEM),
            scratch_shapes=scratch,
            compiler_params=pltpu.CompilerParams(collective_id=0, has_side_effects=True, vmem_limit_bytes=56000000),
        )(*[pltpu.with_memory_space_constraint(a, pltpu.HBM) for a in args])

    return jax.shard_map(device_step, mesh=mesh, in_specs=in_specs, out_specs=P(tok_axes, None), check_vma=False)
```
